64 devices in a mesh: data: 4 (over x, y), cp: 16 (over z, core).
Axes of the slice: x: 2, y: 2, z: 8, core: 2. Of those that a mesh axis runs over, the one named last changes fastest.
The devices are a block of a 4x4x8 slice.
Arguments:
- x_new: bfloat16 [32768, 1536], P(('data', 'cp')), parts along dimension 0
- pos_new: int32 [32768], P(('data', 'cp')), parts along dimension 0
- k_cache: bfloat16 [262144, 2, 128], P(('data', 'cp')), parts along dimension 0
- v_cache: bfloat16 [262144, 2, 128], P(('data', 'cp')), parts along dimension 0
- w_q: bfloat16 [1536, 1536], replicated
- w_k: bfloat16 [1536, 256], replicated
- w_v: bfloat16 [1536, 256], replicated
- w_o: bfloat16 [1536, 1536], replicated
Outputs:
- output: bfloat16 [32768, 1536], P(('data', 'cp')), parts along dimension 0
There are 4 independent parts. The reference program is written for one: setup_inputs(seed, part) draws one part's arguments, and reference() takes and returns one part's arrays. A program takes and returns all parts, laid end to end along the dimension named above; an argument that names none is the same for every part.
All inputs are finite; a program needn't handle non-finite values.
Results may differ from the reference program's by a relative error of at most 0.0054015.
Values are sent between devices in bfloat16 or wider.
A program may use at most 768 MiB of HBM per device.

```python
import math
import numpy as np
import jax
import jax.numpy as jnp
from jax import lax

CP_SIZE = 16
TOK_DEV = 512
CACHE_DEV = 4096
MODEL_DIM = 1536
Q_HEADS = 12
KV_HEADS = 2
HEAD_DIM = 128
ROPE_BASE = 500000
Q_BLOCK = 8

TOKENS = CP_SIZE * TOK_DEV
CACHE_LEN = CP_SIZE * CACHE_DEV
GROUP_SIZE = Q_HEADS // KV_HEADS


def plain_order():
    half_dev = TOK_DEV // 2
    row_idx = np.arange(TOKENS)
    device = row_idx // TOK_DEV
    local_idx = row_idx % TOK_DEV
    piece_idx = np.where(local_idx < half_dev, device, 2 * CP_SIZE - 1 - device)
    return (piece_idx * half_dev + local_idx % half_dev).astype(np.int32)


def rotary(values, positions):
    half_dim = HEAD_DIM // 2
    inv_freq = jnp.power(jnp.float32(ROPE_BASE), -(jnp.arange(half_dim, dtype=jnp.float32) * 2.0 / HEAD_DIM))
    angles = positions.astype(jnp.float32)[:, None] * inv_freq[None, :]
    cos_a = jnp.cos(angles)[:, None, :]
    sin_a = jnp.sin(angles)[:, None, :]
    low_half = values[..., :half_dim]
    high_half = values[..., half_dim:]
    return jnp.concatenate([low_half * cos_a - high_half * sin_a, high_half * cos_a + low_half * sin_a], axis=-1)


def setup_inputs(seed: int = 0, part: int = 0) -> dict:
    part_keys = jax.random.split(jax.random.fold_in(jax.random.key(seed), part), 8)
    weight_keys = jax.random.split(jax.random.key(seed + 1), 4)
    token_order = plain_order()
    walk_x = jnp.cumsum(jax.random.normal(part_keys[0], (TOKENS, MODEL_DIM), jnp.float32), axis=0) / math.sqrt(TOKENS)
    x_plain = walk_x + 0.7 * jax.random.normal(part_keys[1], (TOKENS, MODEL_DIM), jnp.float32)
    start_pos = jax.random.randint(part_keys[2], (), CACHE_LEN, 2 * CACHE_LEN, dtype=jnp.int32)
    positions = start_pos + jnp.asarray(token_order)
    cache_shape = (CACHE_LEN, KV_HEADS, HEAD_DIM)
    walk_k = jnp.cumsum(jax.random.normal(part_keys[3], cache_shape, jnp.float32), axis=0) / math.sqrt(CACHE_LEN)
    walk_v = jnp.cumsum(jax.random.normal(part_keys[4], cache_shape, jnp.float32), axis=0) / math.sqrt(CACHE_LEN)
    k_cache = walk_k + 0.4 * jax.random.normal(part_keys[5], cache_shape, jnp.float32)
    v_cache = 1.2 * walk_v + 0.5 * jax.random.normal(part_keys[6], cache_shape, jnp.float32)
    q_width = Q_HEADS * HEAD_DIM
    kv_width = KV_HEADS * HEAD_DIM
    w_q = jax.random.normal(weight_keys[0], (MODEL_DIM, q_width), jnp.float32) / math.sqrt(MODEL_DIM)
    w_k = 1.5 * jax.random.normal(weight_keys[1], (MODEL_DIM, kv_width), jnp.float32) / math.sqrt(MODEL_DIM)
    w_v = jax.random.normal(weight_keys[2], (MODEL_DIM, kv_width), jnp.float32) / math.sqrt(MODEL_DIM)
    w_o = jax.random.normal(weight_keys[3], (q_width, MODEL_DIM), jnp.float32) / math.sqrt(q_width)
    return {
        "x_new": x_plain[token_order].astype(jnp.bfloat16),
        "pos_new": positions,
        "k_cache": k_cache.astype(jnp.bfloat16),
        "v_cache": v_cache.astype(jnp.bfloat16),
        "w_q": w_q.astype(jnp.bfloat16),
        "w_k": w_k.astype(jnp.bfloat16),
        "w_v": w_v.astype(jnp.bfloat16),
        "w_o": w_o.astype(jnp.bfloat16),
    }


def reference(x_new, pos_new, k_cache, v_cache, w_q, w_k, w_v, w_o):
    q_proj = jnp.dot(x_new, w_q, preferred_element_type=jnp.float32).astype(jnp.bfloat16)
    k_proj = jnp.dot(x_new, w_k, preferred_element_type=jnp.float32).astype(jnp.bfloat16)
    v_new = jnp.dot(x_new, w_v, preferred_element_type=jnp.float32).astype(jnp.bfloat16).reshape(TOKENS, KV_HEADS, HEAD_DIM)
    q_rot = rotary(q_proj.astype(jnp.float32).reshape(TOKENS, Q_HEADS, HEAD_DIM), pos_new).astype(jnp.bfloat16)
    k_new = rotary(k_proj.astype(jnp.float32).reshape(TOKENS, KV_HEADS, HEAD_DIM), pos_new).astype(jnp.bfloat16)
    keys_all = jnp.concatenate([k_cache, k_new], axis=0).astype(jnp.float32)
    vals_all = jnp.concatenate([v_cache, v_new], axis=0).astype(jnp.float32)
    key_pos = jnp.concatenate([jnp.full((CACHE_LEN,), -1, jnp.int32), pos_new])
    score_scale = 1.0 / math.sqrt(HEAD_DIM)
    q_blocks = q_rot.reshape(TOKENS // Q_BLOCK, Q_BLOCK, KV_HEADS, GROUP_SIZE, HEAD_DIM)
    pos_blocks = pos_new.reshape(TOKENS // Q_BLOCK, Q_BLOCK)

    def attend(block_args):
        q_blk, q_pos = block_args
        scores = jnp.einsum("qkgd,ckd->qkgc", q_blk.astype(jnp.float32), keys_all) * score_scale
        visible = key_pos[None, :] <= q_pos[:, None]
        scores = jnp.where(visible[:, None, None, :], scores, -jnp.inf)
        row_max = jnp.max(scores, axis=-1, keepdims=True)
        exp_scores = jnp.exp(scores - row_max)
        row_sum = jnp.sum(exp_scores, axis=-1)
        prob_bf16 = exp_scores.astype(jnp.bfloat16).astype(jnp.float32)
        weighted = jnp.einsum("qkgc,ckd->qkgd", prob_bf16, vals_all)
        return (weighted / row_sum[..., None]).astype(jnp.bfloat16)

    attn_out = lax.map(attend, (q_blocks, pos_blocks)).reshape(TOKENS, Q_HEADS * HEAD_DIM)
    proj_out = jnp.dot(attn_out, w_o, preferred_element_type=jnp.float32)
    return (x_new.astype(jnp.float32) + proj_out).astype(jnp.bfloat16)
```

```python
import functools
import math
import jax
import jax.numpy as jnp
from jax import lax
from jax.experimental import pallas as pl
from jax.experimental.pallas import tpu as pltpu
from jax.sharding import PartitionSpec as P

ROPE_BASE = 500000.0
BLK = 256
HBM = pltpu.HBM
VMEM = pltpu.VMEM
BF16 = jnp.bfloat16
F32 = jnp.float32
MESH_ID = pl.DeviceIdType.MESH
NEG = -1e30
LAG = 2


class Ring:
    def __init__(self, n):
        self.n = n
        me = lax.axis_index("cp")
        self.me = me
        self.sib = me + 1 - 2 * lax.rem(me, 2)
        self.right = lax.rem(me + 2, n)
        self.left = lax.rem(me + n - 2, n)
        self.hops = n // 4
        self.rounds = 4 * (self.hops - 1) + 2
        self.phases = 8 + 4 * self.rounds

    def round_of(self, p):
        return (p - 8) // 4 + 1, lax.rem(p - 8, 4)

    def left_piece(self, base, r):
        s = (r - 1) // 4 + 1
        return lax.rem(base + self.n - 2 * s, self.n), lax.rem(r - 1, 4)

    def right_piece(self, base, r):
        s = (r - 1) // 4 + 1
        return lax.rem(base + 2 * s, self.n), lax.rem(r + 1, 4)

    def piece(self, p):
        r, i = self.round_of(jnp.maximum(p, 8))
        base = jnp.where(i >= 2, self.sib, self.me)
        s = (r - 1) // 4 + 1
        from_right = lax.rem(i, 2)
        dev = lax.rem(base + self.n + (2 * from_right - 1) * 2 * s, self.n)
        j = lax.rem(r - 1 + 2 * from_right, 4)
        early_dev = jnp.where(p >= 4, self.sib, self.me)
        return jnp.where(p < 8, early_dev, dev), jnp.where(p < 8, lax.rem(p, 4), j)

    def head(self, p):
        return self.piece(p)[1] // 2


def dot(a, b):
    return jnp.dot(a, b, preferred_element_type=F32)


def attend_kernel(n, nsb, pairs, scale2, q_in, k_in, v_in, nk_in, nv_in,
                  acc_out, l_out, k_all, v_all, nk_all, nv_all,
                  q_scr, kslot, vslot, nkslot, nvslot, p_scr, kfirst, ones_scr,
                  recv_sem, right_sem, left_sem, sib_sem, own_sib_sem, nrecv_sem, nsend_sem, load_sem, misc_sem, nload_sem):
    ring = Ring(n)
    me, sib, right, left, hops = ring.me, ring.sib, ring.right, ring.left, ring.hops
    rounds, phases = ring.rounds, ring.phases
    tiles = q_scr.shape[0]
    head_tiles = tiles // 2

    def const(value):
        return 0 * me + value

    def send(src, dst, send_sem, recv, to):
        return pltpu.make_async_remote_copy(src_ref=src, dst_ref=dst, send_sem=send_sem, recv_sem=recv,
                                            device_id={"cp": to}, device_id_type=MESH_ID)

    def send_piece(from_own, dev, j, pair_sem, phase, to):
        ksrc = k_in.at[j] if from_own else k_all.at[dev, j]
        vsrc = v_in.at[j] if from_own else v_all.at[dev, j]
        return (send(ksrc, k_all.at[dev, j], pair_sem.at[0], recv_sem.at[phase - 4, 0], to),
                send(vsrc, v_all.at[dev, j], pair_sem.at[1], recv_sem.at[phase - 4, 1], to))

    def send_new(from_own, dev, lo, num, idx, ridx, to):
        ksrc = (nk_in if from_own else nk_all.at[dev]).at[pl.ds(lo, num)]
        vsrc = (nv_in if from_own else nv_all.at[dev]).at[pl.ds(lo, num)]
        return (send(ksrc, nk_all.at[dev, pl.ds(lo, num)], nsend_sem.at[idx, 0], nrecv_sem.at[ridx, 0], to),
                send(vsrc, nv_all.at[dev, pl.ds(lo, num)], nsend_sem.at[idx, 1], nrecv_sem.at[ridx, 1], to))

    def start(copies):
        for c in copies:
            c.start()

    def recv_wait(phase, dev, j):
        for c in send_piece(False, dev, j, right_sem.at[0], phase, me):
            c.wait_recv()

    def nleft(s):
        return lax.rem(me + n - 2 * s, n)

    def nright(s):
        return lax.rem(me + 2 * s, n)

    def nwait(s, side, from_sib):
        base = sib if from_sib else me
        dev = lax.rem(base + (2 * s if side else n - 2 * s), n)
        lo, num = (0, 4) if s < hops else (2 * side, 2)
        for c in send_new(False, dev, lo, num, 0, 2 * (s - 1) + side + (2 * hops if from_sib else 0), me):
            c.wait_recv()

    nsends = []

    def new_step(s):
        for side in (0, 1):
            nwait(s, side, False)
        for side in (0, 1):
            dev = nright(s) if side else nleft(s)
            if s < hops:
                lo, num = (0, 4) if s + 1 < hops else (2 * side, 2)
                idx = len(nsends)
                copies = send_new(False, dev, lo, num, idx, 2 * s + side, left if side else right)
                start(copies)
                nsends.append(num)
            lo, num = (0, 4) if s < hops else (2 * side, 2)
            idx = len(nsends)
            copies = send_new(False, dev, lo, num, idx, 2 * hops + 2 * (s - 1) + side, sib)
            start(copies)
            nsends.append(num)

    barrier = pltpu.get_barrier_semaphore()
    for other in (left, right, sib):
        pl.semaphore_signal(barrier, inc=1, device_id={"cp": other}, device_id_type=MESH_ID)
    pl.semaphore_wait(barrier, 3)

    for other, ridx in ((right, 0), (left, 1), (sib, 4 * hops)):
        start(send_new(True, me, 0, 4, len(nsends), ridx, other))
        nsends.append(4)
    for slot in (1, 2, 3):
        start(send_piece(True, me, slot - 1, right_sem.at[slot % 4], 8 + 4 * (slot - 1), right))
        start(send_piece(True, me, (slot + 1) % 4, left_sem.at[slot % 4], 8 + 4 * (slot - 1) + 1, left))
    for j in range(4):
        start(send_piece(True, me, j, own_sib_sem.at[j], 4 + j, sib))

    def load_piece(own, p, dev, j):
        ksrc = k_in.at[j] if own else k_all.at[dev, j]
        vsrc = v_in.at[j] if own else v_all.at[dev, j]
        slot = lax.rem(p, 4)
        return (pltpu.make_async_copy(ksrc, kslot.at[slot], load_sem.at[slot, 0]),
                pltpu.make_async_copy(vsrc, vslot.at[slot], load_sem.at[slot, 1]))

    first = [pltpu.make_async_copy(q_in, q_scr.at[:, pl.ds(0, BLK // 2)], misc_sem.at[0])]
    first += [pltpu.make_async_copy(k_in.at[2 * h, 0], kfirst.at[h], misc_sem.at[1 + h]) for h in (0, 1)]
    start(first)
    start(load_piece(True, const(0), me, 0))

    ones_scr[...] = jnp.where(lax.broadcasted_iota(jnp.int32, ones_scr.shape, 1) == 0, 1.0, 0.0).astype(BF16)

    def clear(t, _):
        q_scr[t, pl.ds(BLK // 2, BLK // 2)] = jnp.zeros((BLK // 2, BLK), BF16)
        acc_out[t] = jnp.zeros(acc_out.shape[1:], F32)
        l_out[t] = jnp.zeros(l_out.shape[1:], F32)
        return 0
    lax.fori_loop(0, tiles, clear, 0)
    for c in first:
        c.wait()

    def lhs_keys(keys):
        ones = ones_scr[...]
        return jnp.concatenate([keys, jnp.concatenate([ones] * (BLK // 16), axis=0)], axis=1)

    def attend(blocks):
        def scores(b):
            lhs = lhs_keys(b[1]())
            return [dot(lhs, q_scr[b[0] + x]) for x in (0, 1)]

        ahead = scores(blocks[0])
        sums, out = [None, None], [None, None]
        for i in range(len(blocks) + LAG):
            now = ahead
            if i + 1 < len(blocks):
                ahead = scores(blocks[i + 1])
            if i < len(blocks):
                t, _, _, bias, first, last = blocks[i]
                for x in (0, 1):
                    s = now[x] * scale2
                    e = jnp.exp2(s if bias is None else jnp.where(bias, s, NEG))
                    p_scr[x, i % 4] = e.astype(BF16)
                    part = e.reshape(BLK // 8, 8, BLK).sum(axis=0)
                    sums[x] = part if first else sums[x] + part
                    if last:
                        l_out[t + x] = l_out[t + x] + sums[x]
            if i >= LAG:
                t, _, values, _, first, last = blocks[i - LAG]
                v = values()
                for x in (0, 1):
                    part = dot(v, p_scr[x, (i - LAG) % 4])
                    out[x] = part if first else out[x] + part
                    if last:
                        acc_out[t + x] = acc_out[t + x] + out[x]

    def reference_point(i, _):
        lhs = lhs_keys(kfirst[i // 2])
        rows = lax.broadcasted_iota(jnp.int32, (16, BLK), 0)
        for t in range(pairs):
            top = jnp.max(dot(lhs, q_scr[i * pairs + t]), axis=0, keepdims=True)
            q_scr[i * pairs + t, pl.ds(BLK // 2, 16)] = jnp.where(rows == 0, -top, 0.0).astype(BF16)
        return 0
    lax.fori_loop(0, tiles // pairs, reference_point, 0)

    def get_ready(p):
        dev, j = ring.piece(p)

        @pl.when(p < 4)
        def _():
            start(load_piece(True, p, me, j))

        @pl.when(p >= 4)
        def _():
            recv_wait(p, dev, j)
            start(load_piece(False, p, dev, j))
        r, i = ring.round_of(jnp.maximum(p, 8))

        for s, at in new_steps:
            @pl.when(p == at)
            def _():
                new_step(s)

        for side in (0, 1):
            @pl.when((p >= 8) & (i == side))
            def _():
                sem = sib_sem.at[side, lax.rem(r, 2)]

                @pl.when(r > 2)
                def _():
                    for c in send_piece(False, dev, j, sem, p + 2, sib):
                        c.wait_send()
                start(send_piece(False, dev, j, sem, p + 2, sib))
                pool, to = (left_sem, left) if side else (right_sem, right)
                slot = r + 3
                pair_sem = pool.at[lax.rem(slot, 4)]
                phase = 8 + 4 * (slot - 1) + side

                @pl.when(r == 1)
                def _():
                    start(send_piece(True, me, 1 if side else 3, pair_sem, phase, to))

                @pl.when((r > 1) & (slot <= rounds))
                def _():
                    odev, oj = (ring.right_piece if side else ring.left_piece)(me, r - 1)
                    copies = send_piece(False, odev, oj, pair_sem, phase, to)
                    for c in copies:
                        c.wait_send()
                    start(copies)

    def run_phase(p, _):
        dev, j = ring.piece(p)
        for c in load_piece(False, p, dev, j):
            c.wait()

        @pl.when(p + 1 < phases)
        def _():
            get_ready(p + 1)

        @pl.when(p == new_at)
        def _():
            run_new()
        slot = lax.rem(p, 4)
        t0 = (j // 2) * head_tiles
        attend([(t0 + 2 * u, lambda k=k: kslot[slot, k], lambda k=k: vslot[slot, k], None, k == 0, k == nsb - 1)
                for u in range(pairs) for k in range(nsb)])
        return 0

    def run_new():
        for s in range(1, hops + 1):
            for side in (0, 1):
                nwait(s, side, True)
        for c in send_new(False, sib, 0, 4, 0, 4 * hops, me):
            c.wait_recv()

        def loads(d):
            dev = lax.rem(me + d, n)
            return (pltpu.make_async_copy(nk_all.at[dev], nkslot.at[dev], nload_sem.at[d, 0]),
                    pltpu.make_async_copy(nv_all.at[dev], nvslot.at[dev], nload_sem.at[d, 1]))

        def start_loads(d, _):
            start(loads(d))
            return 0

        def wait_loads(d, _):
            for c in loads(d):
                c.wait()
            return 0
        start((pltpu.make_async_copy(nk_in, nkslot.at[me], nload_sem.at[0, 0]),
               pltpu.make_async_copy(nv_in, nvslot.at[me], nload_sem.at[0, 1])))
        lax.fori_loop(1, n, start_loads, 0)
        lax.fori_loop(0, n, wait_loads, 0)
        groups_lo = me // 4 + 1
        groups = n // 2 + 1
        rowcol = (lax.broadcasted_iota(jnp.int32, (BLK, BLK), 0) - lax.broadcasted_iota(jnp.int32, (BLK, BLK), 1))

        def group(u, _):
            h, grp = u // groups, lax.rem(u, groups)
            upper = (grp >= groups_lo).astype(jnp.int32)
            t0 = h * head_tiles + upper * (head_tiles // 2)
            own = jnp.where(upper == 1, 2 * n - 1 - me, me)
            block0 = 4 * jnp.where(upper == 1, grp - groups_lo, grp)
            blocks = []
            for trio in range(pairs // 2):
                for k in range(4):
                    block = block0 + k
                    at = jnp.where(block < n, block, 2 * n - 1 - block)
                    i = 2 * h + (block >= n).astype(jnp.int32)
                    blocks.append((t0 + 2 * trio, lambda at=at, i=i: nkslot[at, i], lambda at=at, i=i: nvslot[at, i],
                                   rowcol <= (own - block) * BLK, k == 0, k == 3))
            attend(blocks)
            return 0
        lax.fori_loop(0, 2 * groups, group, 0)

    new_at = 8 + 4 * (rounds - 4)
    new_steps = [(1, 3), (2, 16), (3, 28), (4, 40)] if hops == 4 else [(s + 1, 3 + s) for s in range(hops)]
    lax.fori_loop(0, phases, run_phase, 0)

    for idx, num in enumerate(nsends):
        for c in send_new(True, me, 0, num, idx, 0, me):
            c.wait_send()
    for slot in range(rounds - 3, rounds + 1):
        for pool in (right_sem, left_sem):
            for c in send_piece(True, me, 0, pool.at[slot % 4], 4, me):
                c.wait_send()
    for side in (0, 1):
        for r in (rounds - 1, rounds):
            for c in send_piece(True, me, 0, sib_sem.at[side, r % 2], 4, me):
                c.wait_send()
    for j in range(4):
        for c in send_piece(True, me, j, own_sib_sem.at[j], 4, me):
            c.wait_send()


def guard_kernel(n, nsb, scale, q_ref, acc_ref, l_ref, k_in, v_in, nk_in, nv_in, k_all, v_all, nk_all, nv_all,
                 o_ref, kbuf, vbuf, m_scr, l_scr, acc_scr, sem):
    me = lax.axis_index("cp")
    tiles = q_ref.shape[0]
    head_tiles = tiles // 2

    def tile(t, _):
        denom = jnp.sum(l_ref[t], axis=0, keepdims=True)
        acc = acc_ref[t]
        fine = (jnp.abs(acc) < jnp.inf) & (denom > 2.0 ** -60) & (denom < 2.0 ** 100)
        o_ref[t] = (acc / denom).astype(BF16)
        faults = jnp.sum(jnp.where(fine, 0.0, 1.0))

        @pl.when(faults > 0.0)
        def _():
            h = t // head_tiles
            upper = lax.rem(t, head_tiles) // (head_tiles // 2)
            own = jnp.where(upper == 1, 2 * n - 1 - me, me)
            m_scr[...] = jnp.full(m_scr.shape, NEG, F32)
            l_scr[...] = jnp.zeros_like(l_scr)
            acc_scr[...] = jnp.zeros_like(acc_scr)

            def fetch(k_src, v_src):
                copies = (pltpu.make_async_copy(k_src, kbuf, sem.at[0]), pltpu.make_async_copy(v_src, vbuf, sem.at[1]))
                for c in copies:
                    c.start()
                for c in copies:
                    c.wait()

            def step(limit):
                s = jnp.dot(kbuf[...], q_ref[t], preferred_element_type=F32) * scale
                rows = lax.broadcasted_iota(jnp.int32, s.shape, 0) - lax.broadcasted_iota(jnp.int32, s.shape, 1)
                seen = rows <= limit
                s = jnp.where(seen, s, -jnp.inf)
                m_old = m_scr[...]
                m_new = jnp.maximum(m_old, jnp.max(s, axis=0, keepdims=True))
                e = jnp.exp(s - m_new)
                old = jnp.exp(m_old - m_new)
                m_scr[...] = m_new
                l_scr[...] = l_scr[...] * old + jnp.sum(e, axis=0, keepdims=True)
                acc_scr[...] = acc_scr[...] * old + jnp.dot(vbuf[...], e.astype(BF16), preferred_element_type=F32)

            def cached(b, _):
                dev, rem = b // (2 * nsb), lax.rem(b, 2 * nsb)
                j, k = 2 * h + rem // nsb, lax.rem(rem, nsb)

                @pl.when(dev == me)
                def _():
                    fetch(k_in.at[j, k], v_in.at[j, k])

                @pl.when(dev != me)
                def _():
                    fetch(k_all.at[dev, j, k], v_all.at[dev, j, k])
                step(0 * me + BLK)
                return 0

            def new(b, _):
                dev = jnp.where(b < n, b, 2 * n - 1 - b)
                j = 2 * h + (b >= n).astype(jnp.int32)

                @pl.when(dev == me)
                def _():
                    fetch(nk_in.at[j], nv_in.at[j])

                @pl.when(dev != me)
                def _():
                    fetch(nk_all.at[dev, j], nv_all.at[dev, j])
                step((own - b) * BLK)
                return 0
            lax.fori_loop(0, 2 * nsb * n, cached, 0)
            lax.fori_loop(0, own + 1, new, 0)
            o_ref[t] = (acc_scr[...] / l_scr[...]).astype(BF16)
        return 0
    lax.fori_loop(0, tiles, tile, 0)


def rotate(low, high, cos_a, sin_a):
    return low * cos_a - high * sin_a, high * cos_a + low * sin_a


def solution(mesh):
    n = mesh.shape["cp"]

    def local_step(x_loc, pos_loc, k_loc, v_loc, w_q, w_k, w_v, w_o):
        tok_dev, model_dim = x_loc.shape
        cache_dev, kv_heads, head_dim = k_loc.shape
        q_heads = w_q.shape[1] // head_dim
        group = q_heads // kv_heads
        half = head_dim // 2
        nsb = cache_dev // (2 * BLK)
        pairs = group
        tiles = 2 * q_heads
        inv_freq = jnp.power(jnp.float32(ROPE_BASE), -(jnp.arange(half, dtype=F32) * 2.0 / head_dim))
        angles = inv_freq[:, None] * pos_loc.astype(F32)[None, :]
        cos_t, sin_t = jnp.cos(angles), jnp.sin(angles)

        k_pieces = jnp.transpose(k_loc, (1, 0, 2)).reshape(4, nsb, BLK, head_dim)
        v_pieces = jnp.transpose(v_loc.reshape(2, nsb, BLK, kv_heads, head_dim), (3, 0, 1, 4, 2)).reshape(4, nsb, head_dim, BLK)

        q_t = lax.dot_general(w_q, x_loc, (((0,), (1,)), ((), ())), preferred_element_type=F32).astype(BF16).astype(F32)
        q_t = q_t.reshape(q_heads, head_dim, tok_dev)
        low, high = rotate(q_t[:, :half], q_t[:, half:], cos_t[None], sin_t[None])
        q_t = jnp.concatenate([low, high], axis=1).astype(BF16)
        q_tiles = jnp.transpose(q_t.reshape(kv_heads, group, head_dim, 2, BLK), (0, 3, 1, 2, 4)).reshape(tiles, head_dim, BLK)

        k_new = jnp.dot(x_loc, w_k, preferred_element_type=F32).astype(BF16).astype(F32).reshape(tok_dev, kv_heads, head_dim)
        low, high = rotate(k_new[..., :half], k_new[..., half:], cos_t.T[:, None, :], sin_t.T[:, None, :])
        k_new = jnp.concatenate([low, high], axis=-1).astype(BF16)
        nk = jnp.transpose(k_new, (1, 0, 2)).reshape(4, BLK, head_dim)
        v_new = lax.dot_general(w_v, x_loc, (((0,), (1,)), ((), ())), preferred_element_type=F32).astype(BF16)
        nv = jnp.transpose(v_new.reshape(kv_heads, head_dim, 2, BLK), (0, 2, 1, 3)).reshape(4, head_dim, BLK)

        hops = n // 4
        rounds = 4 * (hops - 1) + 2
        phases = 8 + 4 * rounds
        any_spec = pl.BlockSpec(memory_space=pl.ANY)
        vmem_spec = pl.BlockSpec(memory_space=VMEM)
        dma = pltpu.SemaphoreType.DMA
        scale2 = math.log2(math.e) / math.sqrt(head_dim)
        n_new_sends = 3 + 2 * (hops - 1) + 2 * hops
        acc, l, k_all, v_all, nk_all, nv_all = pl.pallas_call(
            functools.partial(attend_kernel, n, nsb, pairs, scale2),
            out_shape=(
                jax.ShapeDtypeStruct((tiles, head_dim, BLK), F32),
                jax.ShapeDtypeStruct((tiles, 8, BLK), F32),
                jax.ShapeDtypeStruct((n,) + k_pieces.shape, BF16),
                jax.ShapeDtypeStruct((n,) + v_pieces.shape, BF16),
                jax.ShapeDtypeStruct((n,) + nk.shape, BF16),
                jax.ShapeDtypeStruct((n,) + nv.shape, BF16),
            ),
            in_specs=[any_spec] * 5,
            out_specs=(vmem_spec, vmem_spec, any_spec, any_spec, any_spec, any_spec),
            scratch_shapes=[
                VMEM((tiles, BLK, BLK), BF16),
                VMEM((4, nsb, BLK, head_dim), BF16),
                VMEM((4, nsb, head_dim, BLK), BF16),
                VMEM((n, 4, BLK, head_dim), BF16),
                VMEM((n, 4, head_dim, BLK), BF16),
                VMEM((2, 4, BLK, BLK), BF16),
                VMEM((2, BLK, head_dim), BF16),
                VMEM((16, head_dim), BF16),
                dma((phases - 4, 2)),
                dma((4, 2)),
                dma((4, 2)),
                dma((2, 2, 2)),
                dma((4, 2)),
                dma((4 * hops + 1, 2)),
                dma((n_new_sends, 2)),
                dma((4, 2)),
                dma((3,)),
                dma((n, 2)),
            ],
            compiler_params=pltpu.CompilerParams(collective_id=0, has_side_effects=True, vmem_limit_bytes=56 * 2 ** 20),
            name="ring_attention",
        )(q_tiles, k_pieces, v_pieces, nk, nv)

        o_t = pl.pallas_call(
            functools.partial(guard_kernel, n, nsb, 1.0 / math.sqrt(head_dim)),
            out_shape=jax.ShapeDtypeStruct((tiles, head_dim, BLK), BF16),
            in_specs=[vmem_spec] * 3 + [any_spec] * 8,
            out_specs=vmem_spec,
            scratch_shapes=[VMEM((BLK, head_dim), BF16), VMEM((head_dim, BLK), BF16), VMEM((1, BLK), F32), VMEM((1, BLK), F32),
                            VMEM((head_dim, BLK), F32), dma((2,))],
            compiler_params=pltpu.CompilerParams(vmem_limit_bytes=24 * 2 ** 20),
            name="guard",
        )(q_tiles, acc, l, k_pieces, v_pieces, nk, nv, k_all, v_all, nk_all, nv_all)

        o_t = o_t.reshape(kv_heads, 2, group, head_dim, BLK)
        w_out = w_o.reshape(kv_heads, group, head_dim, model_dim)
        proj = jnp.einsum("kygdt,kgde->yte", o_t, w_out, preferred_element_type=F32).reshape(tok_dev, model_dim)
        return (x_loc.astype(F32) + proj).astype(BF16)

    tok_spec = P(("data", "cp"), None)
    pos_spec = P(("data", "cp"))
    cache_spec = P(("data", "cp"), None, None)
    return jax.shard_map(local_step, mesh=mesh, in_specs=(tok_spec, pos_spec, cache_spec, cache_spec, P(), P(), P(), P()), out_specs=tok_spec, check_vma=False)
```

```python
import functools
import math
import jax
import jax.numpy as jnp
from jax import lax
from jax.experimental import pallas as pl
from jax.experimental.pallas import tpu as pltpu
from jax.sharding import PartitionSpec as P

ROPE_BASE = 500000.0
BLK = 256
HBM = pltpu.HBM
VMEM = pltpu.VMEM
BF16 = jnp.bfloat16
F32 = jnp.float32
MESH_ID = pl.DeviceIdType.MESH
NEG = -1e30
SIDES = (0, 1)
LAG = 2


class Ring:
    def __init__(self, n):
        self.n = n
        me = lax.axis_index("cp")
        self.me = me
        self.sib = me + 1 - 2 * lax.rem(me, 2)
        self.right = lax.rem(me + 2, n)
        self.left = lax.rem(me + n - 2, n)
        self.hops = n // 4
        self.rounds = 4 * (self.hops - 1) + 2
        self.phases = 8 + 4 * self.rounds

    def round_of(self, p):
        return (p - 8) // 4 + 1, lax.rem(p - 8, 4)

    def far(self, base, r, side):
        s = (r - 1) // 4 + 1
        return lax.rem(base + self.n + (2 * side - 1) * 2 * s, self.n), lax.rem(r - 1 + 2 * side, 4)

    def piece(self, p):
        r, i = self.round_of(jnp.maximum(p, 8))
        dev, j = self.far(jnp.where(i >= 2, self.sib, self.me), r, lax.rem(i, 2))
        early_dev = jnp.where(p >= 4, self.sib, self.me)
        return jnp.where(p < 8, early_dev, dev), jnp.where(p < 8, lax.rem(p, 4), j)


def dot(a, b):
    return jnp.dot(a, b, preferred_element_type=F32)


def attend_kernel(n, nsb, pairs, scale2, x_in, wq_in, wk_in, wv_in, cos_in, sin_in, k_in, v_in,
                  acc_out, l_out, q_all, k_all, v_all, nk_all, nv_all,
                  q_scr, kslot, vslot, nkslot, nvslot, p_scr, kfirst, ones_scr, x_scr, wq_scr, wkv_scr, cos_scr, sin_scr,
                  recv_sem, way_sem, sib_sem, own_sib_sem, nrecv_sem, nsend_sem, load_sem, misc_sem, nload_sem):
    ring = Ring(n)
    me, sib, right, left, hops = ring.me, ring.sib, ring.right, ring.left, ring.hops
    rounds, phases = ring.rounds, ring.phases
    tiles = q_scr.shape[0]
    head_tiles = tiles // 2

    def const(value):
        return 0 * me + value

    def send(src, dst, send_sem, recv, to):
        return pltpu.make_async_remote_copy(src_ref=src, dst_ref=dst, send_sem=send_sem, recv_sem=recv,
                                            device_id={"cp": to}, device_id_type=MESH_ID)

    def send_piece(from_own, dev, j, pair_sem, phase, to):
        ksrc = k_in.at[j] if from_own else k_all.at[dev, j]
        vsrc = v_in.at[j] if from_own else v_all.at[dev, j]
        return (send(ksrc, k_all.at[dev, j], pair_sem.at[0], recv_sem.at[phase - 4, 0], to),
                send(vsrc, v_all.at[dev, j], pair_sem.at[1], recv_sem.at[phase - 4, 1], to))

    def send_new(from_own, dev, lo, num, idx, ridx, to):
        ksrc = (nkslot if from_own else nk_all).at[dev, pl.ds(lo, num)]
        vsrc = (nvslot if from_own else nv_all).at[dev, pl.ds(lo, num)]
        return (send(ksrc, nk_all.at[dev, pl.ds(lo, num)], nsend_sem.at[idx, 0], nrecv_sem.at[ridx, 0], to),
                send(vsrc, nv_all.at[dev, pl.ds(lo, num)], nsend_sem.at[idx, 1], nrecv_sem.at[ridx, 1], to))

    def start(copies):
        for c in copies:
            c.start()

    def recv_wait(phase, dev, j):
        for c in send_piece(False, dev, j, own_sib_sem.at[0], phase, me):
            c.wait_recv()

    def nleft(s):
        return lax.rem(me + n - 2 * s, n)

    def nright(s):
        return lax.rem(me + 2 * s, n)

    def nwait(s, side, from_sib):
        base = sib if from_sib else me
        dev = lax.rem(base + (2 * s if side else n - 2 * s), n)
        lo, num = (0, 4) if s < hops else (2 * side, 2)
        for c in send_new(False, dev, lo, num, 0, 2 * (s - 1) + side + (2 * hops if from_sib else 0), me):
            c.wait_recv()

    nsends = []

    def new_step(s):
        for side in SIDES:
            nwait(s, side, False)
        for side in SIDES:
            dev = nright(s) if side else nleft(s)
            if s < hops:
                lo, num = (0, 4) if s + 1 < hops else (2 * side, 2)
                idx = len(nsends)
                copies = send_new(False, dev, lo, num, idx, 2 * s + side, left if side else right)
                start(copies)
                nsends.append(num)
            lo, num = (0, 4) if s < hops else (2 * side, 2)
            idx = len(nsends)
            copies = send_new(False, dev, lo, num, idx, 2 * hops + 2 * (s - 1) + side, sib)
            start(copies)
            nsends.append(num)

    barrier = pltpu.get_barrier_semaphore()
    for other in (left, right, sib):
        pl.semaphore_signal(barrier, inc=1, device_id={"cp": other}, device_id_type=MESH_ID)
    pl.semaphore_wait(barrier, 3)

    def own_slot(slot):
        for side in SIDES:
            start(slot_copies(slot, side, True, me, lax.rem(slot - 1 + 2 * side, 4)))

    def slot_copies(slot, side, own, dev, j):
        return send_piece(own, dev, j, way_sem.at[side, lax.rem(slot, 4)], 4 + 4 * slot + side, (right, left)[side])

    own_slot(const(1))
    for j in range(4):
        start(send_piece(True, me, j, own_sib_sem.at[j], 4 + j, sib))

    def load_piece(own, p, dev, j):
        ksrc = k_in.at[j] if own else k_all.at[dev, j]
        vsrc = v_in.at[j] if own else v_all.at[dev, j]
        slot = lax.rem(p, 4)
        return (pltpu.make_async_copy(ksrc, kslot.at[slot], load_sem.at[slot, 0]),
                pltpu.make_async_copy(vsrc, vslot.at[slot], load_sem.at[slot, 1]))

    kv_width = wk_in.shape[1]
    first = [pltpu.make_async_copy(x_in, x_scr, misc_sem.at[0]),
             pltpu.make_async_copy(wk_in, wkv_scr.at[:, pl.ds(0, kv_width)], misc_sem.at[1]),
             pltpu.make_async_copy(wv_in, wkv_scr.at[:, pl.ds(kv_width, kv_width)], misc_sem.at[2]),
             pltpu.make_async_copy(cos_in, cos_scr, misc_sem.at[3]),
             pltpu.make_async_copy(sin_in, sin_scr, misc_sem.at[4])]
    then = [pltpu.make_async_copy(wq_in, wq_scr, misc_sem.at[5])]
    then += [pltpu.make_async_copy(k_in.at[2 * h, 0], kfirst.at[h], misc_sem.at[6 + h]) for h in SIDES]
    start(first)
    start(then)
    start(load_piece(True, const(0), me, 0))

    ones_scr[...] = jnp.where(lax.broadcasted_iota(jnp.int32, ones_scr.shape, 1) == 0, 1.0, 0.0).astype(BF16)

    def clear(t, _):
        q_scr[t, pl.ds(BLK // 2, BLK // 2)] = jnp.zeros((BLK // 2, BLK), BF16)
        acc_out[t] = jnp.zeros(acc_out.shape[1:], F32)
        l_out[t] = jnp.zeros(l_out.shape[1:], F32)
        return 0
    lax.fori_loop(0, tiles, clear, 0)
    for c in first:
        c.wait()

    head_dim = BLK // 2

    def turned(u):
        u = u.astype(BF16).astype(F32)
        return (u * cos_scr[...] + pltpu.roll(u, head_dim // 2, 1) * sin_scr[...]).astype(BF16)

    new_kv = dot(x_scr[...], wkv_scr[...])
    for h in SIDES:
        keys = turned(new_kv[:, h * head_dim:(h + 1) * head_dim])
        values = new_kv[:, kv_width + h * head_dim:kv_width + (h + 1) * head_dim].T.astype(BF16)
        for half in SIDES:
            nkslot[me, 2 * h + half] = keys[half * BLK:(half + 1) * BLK]
            nvslot[me, 2 * h + half] = values[:, half * BLK:(half + 1) * BLK]
    for c in then:
        c.wait()
    heads = 4

    def project(c, _):
        width = heads * head_dim
        z = dot(x_scr[...], wq_scr[:, pl.ds(pl.multiple_of(c * width, width), width)])
        for i in range(heads):
            head = c * heads + i
            t = (head // pairs) * head_tiles + lax.rem(head, pairs)
            u = turned(z[:, i * head_dim:(i + 1) * head_dim]).astype(F32).T.astype(BF16)
            for half in SIDES:
                q_scr[t + half * pairs, pl.ds(0, head_dim)] = u[:, half * BLK:(half + 1) * BLK]
        return 0
    lax.fori_loop(0, tiles // (2 * heads), project, 0)

    for other, ridx in ((right, 0), (left, 1), (sib, 4 * hops)):
        start(send_new(True, me, 0, 4, len(nsends), ridx, other))
        nsends.append(4)
    own_slot(const(2))
    own_slot(const(3))
    kept = [pltpu.make_async_copy(q_scr.at[:, pl.ds(0, head_dim)], q_all, misc_sem.at[8]),
            pltpu.make_async_copy(nkslot.at[me], nk_all.at[me], misc_sem.at[9]),
            pltpu.make_async_copy(nvslot.at[me], nv_all.at[me], misc_sem.at[10])]
    start(kept)

    def lhs_keys(keys):
        ones = ones_scr[...]
        return jnp.concatenate([keys, jnp.concatenate([ones] * (BLK // 16), axis=0)], axis=1)

    def attend(blocks):
        def scores(b):
            lhs = lhs_keys(b[1]())
            return [dot(lhs, q_scr[b[0] + x]) for x in SIDES]

        ahead = scores(blocks[0])
        sums, out = [None, None], [None, None]
        for i in range(len(blocks) + LAG):
            now = ahead
            if i + 1 < len(blocks):
                ahead = scores(blocks[i + 1])
            if i < len(blocks):
                t, _, _, bias, first, last = blocks[i]
                for x in SIDES:
                    s = now[x] * scale2
                    e = jnp.exp2(s if bias is None else jnp.where(bias, s, NEG))
                    p_scr[x, i % 4] = e.astype(BF16)
                    part = e.reshape(BLK // 8, 8, BLK).sum(axis=0)
                    sums[x] = part if first else sums[x] + part
                    if last:
                        l_out[t + x] = l_out[t + x] + sums[x]
            if i >= LAG:
                t, _, values, _, first, last = blocks[i - LAG]
                v = values()
                for x in SIDES:
                    part = dot(v, p_scr[x, (i - LAG) % 4])
                    out[x] = part if first else out[x] + part
                    if last:
                        acc_out[t + x] = acc_out[t + x] + out[x]

    def reference_point(i, _):
        lhs = lhs_keys(kfirst[i // 2])
        rows = lax.broadcasted_iota(jnp.int32, (16, BLK), 0)
        for t in range(pairs):
            top = jnp.max(dot(lhs, q_scr[i * pairs + t]), axis=0, keepdims=True)
            q_scr[i * pairs + t, pl.ds(BLK // 2, 16)] = jnp.where(rows == 0, -top, 0.0).astype(BF16)
        return 0
    lax.fori_loop(0, tiles // pairs, reference_point, 0)

    def get_ready(p):
        dev, j = ring.piece(p)

        @pl.when(p < 4)
        def _():
            start(load_piece(True, p, me, j))

        @pl.when(p >= 4)
        def _():
            recv_wait(p, dev, j)
            start(load_piece(False, p, dev, j))

        for s, at in enumerate(new_steps):
            @pl.when(p == at)
            def _():
                new_step(s + 1)
        for s, at in enumerate(new_parts):
            @pl.when(p == at)
            def _():
                for side in SIDES:
                    nwait(s + 1, side, True)
                if s == 0:
                    for c in send_new(False, sib, 0, 4, 0, 4 * hops, me):
                        c.wait_recv()

        @pl.when(new_part(p) >= 0)
        def _():
            each_load(new_part(p), lambda c: c.start())
        r, i = ring.round_of(jnp.maximum(p, 8))

        @pl.when((p >= 8) & (i < 2))
        def _():
            copies = send_piece(False, dev, j, sib_sem.at[i, lax.rem(r, 2)], p + 2, sib)

            @pl.when(r > 2)
            def _():
                for c in copies:
                    c.wait_send()
            start(copies)

        @pl.when((p >= 8) & (i == 0) & (r > 1) & (r + 2 <= rounds))
        def _():
            @pl.when(r == 2)
            def _():
                own_slot(r + 2)

            @pl.when(r > 2)
            def _():
                for side in SIDES:
                    copies = slot_copies(r + 2, side, False, *ring.far(me, r - 2, side))
                    for c in copies:
                        c.wait_send()
                    start(copies)

    def run_phase(p, _):
        dev, j = ring.piece(p)
        for c in load_piece(False, p, dev, j):
            c.wait()

        @pl.when(p + 1 < phases)
        def _():
            get_ready(p + 1)

        @pl.when(new_part(p) >= 0)
        def _():
            run_new(new_part(p))
        slot = lax.rem(p, 4)
        t0 = (j // 2) * head_tiles
        attend([(t0 + 2 * u, lambda k=k: kslot[slot, k], lambda k=k: vslot[slot, k], None, k == 0, k == nsb - 1)
                for u in range(pairs) for k in range(nsb)])
        return 0

    quad = me // 4
    quads = n // 4

    def new_part(p):
        part = const(-1)
        for s, at in enumerate(new_parts):
            part = jnp.where(p == at, s, part)
        return part

    def part_quad(part):
        near = jnp.where(lax.rem(me // 2, 2) == 0, -1, 1)
        step = jnp.where(part == 1, near, jnp.where(part == 2, -near, part // 3 * 2))
        return lax.rem(quad + step + quads, quads)

    def each_load(part, do):
        m = part_quad(part)
        for d in range(4):
            dev = 4 * m + d

            @pl.when(dev != me)
            def _():
                do(pltpu.make_async_copy(nk_all.at[dev], nkslot.at[dev], nload_sem.at[d, 0]))
                do(pltpu.make_async_copy(nv_all.at[dev], nvslot.at[dev], nload_sem.at[d, 1]))

    def run_new(part):
        m = part_quad(part)
        each_load(part, lambda c: c.wait())
        rowcol = (lax.broadcasted_iota(jnp.int32, (BLK, BLK), 0) - lax.broadcasted_iota(jnp.int32, (BLK, BLK), 1))

        def group(v, _):
            low_tile = jnp.where(part == 0, v == 0, (v == 1) & (m < quad))
            late_keys = jnp.where(part == 0, v == 2, (v == 1) & (m > quad))
            own = jnp.where(low_tile, me, 2 * n - 1 - me)
            block0 = 4 * jnp.where(late_keys, 2 * quads - 1 - m, m)
            blocks = []
            for h in SIDES:
                t0 = h * head_tiles + jnp.where(low_tile, 0, head_tiles // 2)
                for trio in range(pairs // 2):
                    for k in range(4):
                        block = block0 + k
                        at = jnp.where(late_keys, 2 * n - 1 - block, block)
                        i = 2 * h + late_keys.astype(jnp.int32)
                        blocks.append((t0 + 2 * trio, lambda at=at, i=i: nkslot[at, i], lambda at=at, i=i: nvslot[at, i],
                                       rowcol <= (own - block) * BLK, k == 0, k == 3))
            attend(blocks)
            return 0
        lax.fori_loop(0, jnp.where(part == 0, 3, 2), group, 0)

    new_steps = [8 * s + 9 for s in range(hops)] if hops == 4 else [5, 7]
    new_parts = [13, 22, 29, 37] if hops == 4 else [8, 10]
    lax.fori_loop(0, phases, run_phase, 0)

    for c in kept:
        c.wait()
    for idx, num in enumerate(nsends):
        for c in send_new(True, me, 0, num, idx, 0, me):
            c.wait_send()
    def drain(sem):
        for c in send_piece(True, me, 0, sem, 4, me):
            c.wait_send()
    for side in SIDES:
        for slot in range(4):
            drain(way_sem.at[side, slot])
        for slot in SIDES:
            drain(sib_sem.at[side, slot])
    for slot in range(4):
        drain(own_sib_sem.at[slot])


def output_kernel(n, nsb, pairs, scale, x_ref, acc_ref, l_ref, wo_in, q_all, k_in, v_in, k_all, v_all, nk_all, nv_all,
                  y_ref, wo_scr, o_scr, qbuf, kbuf, vbuf, m_scr, l_scr, acc_scr, sem):
    me = lax.axis_index("cp")
    tiles = acc_ref.shape[0]
    head_tiles = tiles // 2
    head_dim = BLK // 2
    weights = pltpu.make_async_copy(wo_in, wo_scr, sem.at[3])
    weights.start()

    def put(t, o_t):
        h, upper, g = t // head_tiles, lax.rem(t, head_tiles) // pairs, lax.rem(t, pairs)
        rows = pl.ds(pl.multiple_of(upper * BLK, BLK), BLK)
        columns = pl.ds(pl.multiple_of((h * pairs + g) * head_dim, head_dim), head_dim)
        o_scr[rows, columns] = o_t.T.astype(BF16)

    def faults_of(t):
        denom = jnp.sum(l_ref[t], axis=0, keepdims=True)
        acc = acc_ref[t]
        fine = (jnp.abs(acc) < jnp.inf) & (denom > 2.0 ** -60) & (denom < 2.0 ** 100)
        faults = jnp.where(fine, 0.0, 1.0).reshape(head_dim // 8, 8, BLK).sum(axis=0)
        return acc * (1.0 / denom), faults

    def some(i, faults):
        for g in range(pairs):
            o_t, more = faults_of(i * pairs + g)
            put(i * pairs + g, o_t)
            faults = faults + more
        return faults
    faults = lax.fori_loop(0, tiles // pairs, some, jnp.zeros((8, BLK), F32))

    @pl.when(jnp.sum(faults) > 0.0)
    def _():
        def tile(t, _):
            @pl.when(jnp.sum(faults_of(t)[1]) > 0.0)
            def _():
                h = t // head_tiles
                upper = lax.rem(t, head_tiles) // pairs
                own = jnp.where(upper == 1, 2 * n - 1 - me, me)
                m_scr[...] = jnp.full(m_scr.shape, NEG, F32)
                l_scr[...] = jnp.zeros_like(l_scr)
                acc_scr[...] = jnp.zeros_like(acc_scr)
                queries = pltpu.make_async_copy(q_all.at[t], qbuf, sem.at[2])
                queries.start()
                queries.wait()

                def fetch(k_src, v_src):
                    copies = (pltpu.make_async_copy(k_src, kbuf, sem.at[0]), pltpu.make_async_copy(v_src, vbuf, sem.at[1]))
                    for c in copies:
                        c.start()
                    for c in copies:
                        c.wait()

                def step(limit):
                    s = dot(kbuf[...], qbuf[...]) * scale
                    rows = lax.broadcasted_iota(jnp.int32, s.shape, 0) - lax.broadcasted_iota(jnp.int32, s.shape, 1)
                    s = jnp.where(rows <= limit, s, -jnp.inf)
                    m_old = m_scr[...]
                    m_new = jnp.maximum(m_old, jnp.max(s, axis=0, keepdims=True))
                    e = jnp.exp(s - m_new)
                    old = jnp.exp(m_old - m_new)
                    m_scr[...] = m_new
                    l_scr[...] = l_scr[...] * old + jnp.sum(e, axis=0, keepdims=True)
                    acc_scr[...] = acc_scr[...] * old + dot(vbuf[...], e.astype(BF16))

                def cached(b, _):
                    dev, rem = b // (2 * nsb), lax.rem(b, 2 * nsb)
                    j, k = 2 * h + rem // nsb, lax.rem(rem, nsb)

                    @pl.when(dev == me)
                    def _():
                        fetch(k_in.at[j, k], v_in.at[j, k])

                    @pl.when(dev != me)
                    def _():
                        fetch(k_all.at[dev, j, k], v_all.at[dev, j, k])
                    step(0 * me + BLK)
                    return 0

                def new(b, _):
                    dev = jnp.where(b < n, b, 2 * n - 1 - b)
                    j = 2 * h + (b >= n).astype(jnp.int32)
                    fetch(nk_all.at[dev, j], nv_all.at[dev, j])
                    step((own - b) * BLK)
                    return 0
                lax.fori_loop(0, 2 * nsb * n, cached, 0)
                lax.fori_loop(0, own + 1, new, 0)
                put(t, acc_scr[...] / l_scr[...])
            return 0
        lax.fori_loop(0, tiles, tile, 0)
    weights.wait()
    width = min(512, wo_scr.shape[1])

    def project(c, _):
        columns = pl.ds(pl.multiple_of(c * width, width), width)
        y_ref[:, columns] = (x_ref[:, columns].astype(F32) + dot(o_scr[...], wo_scr[:, columns])).astype(BF16)
        return 0
    lax.fori_loop(0, wo_scr.shape[1] // width, project, 0)


def solution(mesh):
    n = mesh.shape["cp"]

    def local_step(x_loc, pos_loc, k_loc, v_loc, w_q, w_k, w_v, w_o):
        tok_dev, model_dim = x_loc.shape
        cache_dev, kv_heads, head_dim = k_loc.shape
        q_heads = w_q.shape[1] // head_dim
        group = q_heads // kv_heads
        half = head_dim // 2
        nsb = cache_dev // (2 * BLK)
        pairs = group
        tiles = 2 * q_heads
        inv_freq = jnp.power(jnp.float32(ROPE_BASE), -(jnp.arange(half, dtype=F32) * 2.0 / head_dim))
        angles = pos_loc.astype(F32)[:, None] * inv_freq[None, :]
        cos_a, sin_a = jnp.cos(angles), jnp.sin(angles)
        cos_t = jnp.concatenate([cos_a, cos_a], axis=1)
        sin_t = jnp.concatenate([-sin_a, sin_a], axis=1)

        k_pieces = jnp.transpose(k_loc, (1, 0, 2)).reshape(4, nsb, BLK, head_dim)
        v_pieces = jnp.transpose(v_loc.reshape(2, nsb, BLK, kv_heads, head_dim), (3, 0, 1, 4, 2)).reshape(4, nsb, head_dim, BLK)

        hops = n // 4
        rounds = 4 * (hops - 1) + 2
        phases = 8 + 4 * rounds
        vmem_spec = pl.BlockSpec(memory_space=VMEM)
        dma = pltpu.SemaphoreType.DMA
        scale2 = math.log2(math.e) / math.sqrt(head_dim)
        n_new_sends = 3 + 2 * (hops - 1) + 2 * hops
        hbm_spec = pl.BlockSpec(memory_space=HBM)
        acc, l, q_all, k_all, v_all, nk_all, nv_all = pl.pallas_call(
            functools.partial(attend_kernel, n, nsb, pairs, scale2),
            out_shape=(
                jax.ShapeDtypeStruct((tiles, head_dim, BLK), F32),
                jax.ShapeDtypeStruct((tiles, 8, BLK), F32),
                jax.ShapeDtypeStruct((tiles, head_dim, BLK), BF16),
                jax.ShapeDtypeStruct((n,) + k_pieces.shape, BF16),
                jax.ShapeDtypeStruct((n,) + v_pieces.shape, BF16),
                jax.ShapeDtypeStruct((n, 4, BLK, head_dim), BF16),
                jax.ShapeDtypeStruct((n, 4, head_dim, BLK), BF16),
            ),
            in_specs=[hbm_spec] * 8,
            out_specs=(vmem_spec, vmem_spec) + (hbm_spec,) * 5,
            scratch_shapes=[
                VMEM((tiles, BLK, BLK), BF16),
                VMEM((4, nsb, BLK, head_dim), BF16),
                VMEM((4, nsb, head_dim, BLK), BF16),
                VMEM((n, 4, BLK, head_dim), BF16),
                VMEM((n, 4, head_dim, BLK), BF16),
                VMEM((2, 4, BLK, BLK), BF16),
                VMEM((2, BLK, head_dim), BF16),
                VMEM((16, head_dim), BF16),
                VMEM(x_loc.shape, BF16),
                VMEM(w_q.shape, BF16),
                VMEM((model_dim, 2 * w_k.shape[1]), BF16),
                VMEM((tok_dev, head_dim), F32),
                VMEM((tok_dev, head_dim), F32),
                dma((phases - 4, 2)),
                dma((2, 4, 2)),
                dma((2, 2, 2)),
                dma((4, 2)),
                dma((4 * hops + 1, 2)),
                dma((n_new_sends, 2)),
                dma((4, 2)),
                dma((11,)),
                dma((4, 2)),
            ],
            compiler_params=pltpu.CompilerParams(collective_id=0, has_side_effects=True, vmem_limit_bytes=48 * 2 ** 20),
            name="ring_attention",
        )(x_loc, w_q, w_k, w_v, cos_t, sin_t, k_pieces, v_pieces)

        return pl.pallas_call(
            functools.partial(output_kernel, n, nsb, pairs, 1.0 / math.sqrt(head_dim)),
            out_shape=jax.ShapeDtypeStruct((tok_dev, model_dim), BF16),
            in_specs=[vmem_spec] * 3 + [hbm_spec] * 8,
            out_specs=vmem_spec,
            scratch_shapes=[VMEM(w_o.shape, BF16), VMEM((tok_dev, q_heads * head_dim), BF16), VMEM((head_dim, BLK), BF16),
                            VMEM((BLK, head_dim), BF16), VMEM((head_dim, BLK), BF16), VMEM((1, BLK), F32), VMEM((1, BLK), F32),
                            VMEM((head_dim, BLK), F32), dma((4,))],
            compiler_params=pltpu.CompilerParams(vmem_limit_bytes=40 * 2 ** 20),
            name="output",
        )(x_loc, acc, l, w_o, q_all, k_pieces, v_pieces, k_all, v_all, nk_all, nv_all)

    tok_spec = P(("data", "cp"), None)
    pos_spec = P(("data", "cp"))
    cache_spec = P(("data", "cp"), None, None)
    return jax.shard_map(local_step, mesh=mesh, in_specs=(tok_spec, pos_spec, cache_spec, cache_spec, P(), P(), P(), P()), out_specs=tok_spec, check_vma=False)
```

```python
import functools
import math
import jax
import jax.numpy as jnp
from jax import lax
from jax.experimental import pallas as pl
from jax.experimental.pallas import tpu as pltpu
from jax.sharding import PartitionSpec as P

ROPE_BASE = 500000.0
BLK = 256
HBM = pltpu.HBM
VMEM = pltpu.VMEM
BF16 = jnp.bfloat16
F32 = jnp.float32
MESH_ID = pl.DeviceIdType.MESH
NEG = -1e30
SIDES = (0, 1)
LAG = 2


class Ring:
    def __init__(self, n):
        self.n = n
        me = lax.axis_index("cp")
        self.me = me
        self.sib = me + 1 - 2 * lax.rem(me, 2)
        self.right = lax.rem(me + 2, n)
        self.left = lax.rem(me + n - 2, n)
        self.hops = n // 4
        self.rounds = 4 * (self.hops - 1) + 2
        self.phases = 8 + 4 * self.rounds

    def round_of(self, p):
        return (p - 8) // 4 + 1, lax.rem(p - 8, 4)

    def far(self, base, r, side):
        s = (r - 1) // 4 + 1
        return lax.rem(base + self.n + (2 * side - 1) * 2 * s, self.n), lax.rem(r - 1 + 2 * side, 4)

    def piece(self, p):
        r, i = self.round_of(jnp.maximum(p, 8))
        dev, j = self.far(jnp.where(i >= 2, self.sib, self.me), r, lax.rem(i, 2))
        early_dev = jnp.where(p >= 4, self.sib, self.me)
        return jnp.where(p < 8, early_dev, dev), jnp.where(p < 8, lax.rem(p, 4), j)


def dot(a, b):
    return jnp.dot(a, b, preferred_element_type=F32)


def attend_kernel(n, nsb, pairs, scale2, x_ref, wq_in, wk_ref, wv_ref, cos_ref, sin_ref, k_in, vn_ref,
                  acc_out, l_out, q_all, k_all, v_all, nk_all, nv_all,
                  q_scr, kslot, vslot, nkslot, nvslot, p_scr, kfirst, ones_scr, wq_scr, vt_scr,
                  recv_sem, way_sem, sib_sem, own_sib_sem, nrecv_sem, nsend_sem, load_sem, misc_sem, nload_sem):
    ring = Ring(n)
    me, sib, right, left, hops = ring.me, ring.sib, ring.right, ring.left, ring.hops
    rounds, phases = ring.rounds, ring.phases
    tiles = q_scr.shape[0]
    head_tiles = tiles // 2

    def const(value):
        return 0 * me + value

    def send(src, dst, send_sem, recv, to):
        return pltpu.make_async_remote_copy(src_ref=src, dst_ref=dst, send_sem=send_sem, recv_sem=recv,
                                            device_id={"cp": to}, device_id_type=MESH_ID)

    def send_piece(from_own, dev, j, pair_sem, phase, to):
        ksrc = k_in.at[j] if from_own else k_all.at[dev, j]
        vsrc = v_all.at[dev, j]
        return (send(ksrc, k_all.at[dev, j], pair_sem.at[0], recv_sem.at[phase - 4, 0], to),
                send(vsrc, v_all.at[dev, j], pair_sem.at[1], recv_sem.at[phase - 4, 1], to))

    def send_new(from_own, dev, lo, num, idx, ridx, to):
        ksrc = (nkslot if from_own else nk_all).at[dev, pl.ds(lo, num)]
        vsrc = (nvslot if from_own else nv_all).at[dev, pl.ds(lo, num)]
        return (send(ksrc, nk_all.at[dev, pl.ds(lo, num)], nsend_sem.at[idx, 0], nrecv_sem.at[ridx, 0], to),
                send(vsrc, nv_all.at[dev, pl.ds(lo, num)], nsend_sem.at[idx, 1], nrecv_sem.at[ridx, 1], to))

    def start(copies):
        for c in copies:
            c.start()

    def recv_wait(phase, dev, j):
        for c in send_piece(False, dev, j, own_sib_sem.at[0], phase, me):
            c.wait_recv()

    def nleft(s):
        return lax.rem(me + n - 2 * s, n)

    def nright(s):
        return lax.rem(me + 2 * s, n)

    def nwait(s, side, from_sib):
        base = sib if from_sib else me
        dev = lax.rem(base + (2 * s if side else n - 2 * s), n)
        lo, num = (0, 4) if s < hops else (2 * side, 2)
        for c in send_new(False, dev, lo, num, 0, 2 * (s - 1) + side + (2 * hops if from_sib else 0), me):
            c.wait_recv()

    nsends = []

    def new_step(s):
        for side in SIDES:
            nwait(s, side, False)
        for side in SIDES:
            dev = nright(s) if side else nleft(s)
            if s < hops:
                lo, num = (0, 4) if s + 1 < hops else (2 * side, 2)
                idx = len(nsends)
                copies = send_new(False, dev, lo, num, idx, 2 * s + side, left if side else right)
                start(copies)
                nsends.append(num)
            lo, num = (0, 4) if s < hops else (2 * side, 2)
            idx = len(nsends)
            copies = send_new(False, dev, lo, num, idx, 2 * hops + 2 * (s - 1) + side, sib)
            start(copies)
            nsends.append(num)

    then = [pltpu.make_async_copy(wq_in, wq_scr, misc_sem.at[0])]
    then += [pltpu.make_async_copy(k_in.at[2 * h, 0], kfirst.at[h], misc_sem.at[1 + h]) for h in SIDES]
    start(then)

    barrier = pltpu.get_barrier_semaphore()
    for other in (left, right, sib):
        pl.semaphore_signal(barrier, inc=1, device_id={"cp": other}, device_id_type=MESH_ID)
    pl.semaphore_wait(barrier, 3)

    def own_slot(slot):
        for side in SIDES:
            start(slot_copies(slot, side, True, me, lax.rem(slot - 1 + 2 * side, 4)))

    def slot_copies(slot, side, own, dev, j):
        return send_piece(own, dev, j, way_sem.at[side, lax.rem(slot, 4)], 4 + 4 * slot + side, (right, left)[side])

    first_round = [slot_copies(const(1), side, True, me, 2 * side) for side in SIDES]
    first_round += [send_piece(True, me, j, own_sib_sem.at[j], 4 + j, sib) for j in range(4)]
    start([c[0] for c in first_round])

    def load_piece(own, p, dev, j):
        ksrc = k_in.at[j] if own else k_all.at[dev, j]
        vsrc = v_all.at[dev, j]
        slot = lax.rem(p, 4)
        return (pltpu.make_async_copy(ksrc, kslot.at[slot], load_sem.at[slot, 0]),
                pltpu.make_async_copy(vsrc, vslot.at[slot], load_sem.at[slot, 1]))

    ones_scr[...] = jnp.where(lax.broadcasted_iota(jnp.int32, ones_scr.shape, 1) == 0, 1.0, 0.0).astype(BF16)

    def clear(t, _):
        q_scr[t, pl.ds(BLK // 2, BLK // 2)] = jnp.zeros((BLK // 2, BLK), BF16)
        acc_out[t] = jnp.zeros(acc_out.shape[1:], F32)
        l_out[t] = jnp.zeros(l_out.shape[1:], F32)
        return 0
    lax.fori_loop(0, tiles, clear, 0)

    def transpose(j, _):
        for k in range(nsb):
            vt_scr[j, k] = vn_ref[j, k].T
        return 0
    lax.fori_loop(0, 4, transpose, 0)
    own_values = pltpu.make_async_copy(vt_scr, v_all.at[me], misc_sem.at[3])
    own_values.start()

    head_dim = BLK // 2

    def turned(u):
        u = u.astype(BF16).astype(F32)
        return (u * cos_ref[...] + pltpu.roll(u, head_dim // 2, 1) * sin_ref[...]).astype(BF16)

    new_k, new_v = dot(x_ref[...], wk_ref[...]), dot(x_ref[...], wv_ref[...])
    for h in SIDES:
        keys = turned(new_k[:, h * head_dim:(h + 1) * head_dim])
        values = new_v[:, h * head_dim:(h + 1) * head_dim].T.astype(BF16)
        for half in SIDES:
            nkslot[me, 2 * h + half] = keys[half * BLK:(half + 1) * BLK]
            nvslot[me, 2 * h + half] = values[:, half * BLK:(half + 1) * BLK]
    own_values.wait()
    start([c[1] for c in first_round])
    start(load_piece(True, const(0), me, 0))
    for c in then:
        c.wait()
    heads = 4

    def project(c, _):
        width = heads * head_dim
        z = dot(x_ref[...], wq_scr[:, pl.ds(pl.multiple_of(c * width, width), width)])
        for i in range(heads):
            head = c * heads + i
            t = (head // pairs) * head_tiles + lax.rem(head, pairs)
            u = turned(z[:, i * head_dim:(i + 1) * head_dim]).astype(F32).T.astype(BF16)
            for half in SIDES:
                q_scr[t + half * pairs, pl.ds(0, head_dim)] = u[:, half * BLK:(half + 1) * BLK]
        return 0
    lax.fori_loop(0, tiles // (2 * heads), project, 0)

    for other, ridx in ((right, 0), (left, 1), (sib, 4 * hops)):
        start(send_new(True, me, 0, 4, len(nsends), ridx, other))
        nsends.append(4)
    own_slot(const(2))
    own_slot(const(3))
    kept = [pltpu.make_async_copy(q_scr.at[:, pl.ds(0, head_dim)], q_all, misc_sem.at[4]),
            pltpu.make_async_copy(nkslot.at[me], nk_all.at[me], misc_sem.at[5]),
            pltpu.make_async_copy(nvslot.at[me], nv_all.at[me], misc_sem.at[6])]
    start(kept)

    def lhs_keys(keys):
        ones = ones_scr[...]
        return jnp.concatenate([keys, jnp.concatenate([ones] * (BLK // 16), axis=0)], axis=1)

    def attend(blocks):
        def scores(b):
            lhs = lhs_keys(b[1]())
            return [dot(lhs, q_scr[b[0] + x]) for x in SIDES]

        ahead = scores(blocks[0])
        sums, out = [None, None], [None, None]
        for i in range(len(blocks) + LAG):
            now = ahead
            if i + 1 < len(blocks):
                ahead = scores(blocks[i + 1])
            if i < len(blocks):
                t, _, _, bias, first, last = blocks[i]
                for x in SIDES:
                    s = now[x] * scale2
                    e = jnp.exp2(s if bias is None else jnp.where(bias, s, NEG))
                    p_scr[x, i % 4] = e.astype(BF16)
                    part = e.reshape(BLK // 8, 8, BLK).sum(axis=0)
                    sums[x] = part if first else sums[x] + part
                    if last:
                        l_out[t + x] = l_out[t + x] + sums[x]
            if i >= LAG:
                t, _, values, _, first, last = blocks[i - LAG]
                v = values()
                for x in SIDES:
                    part = dot(v, p_scr[x, (i - LAG) % 4])
                    out[x] = part if first else out[x] + part
                    if last:
                        acc_out[t + x] = acc_out[t + x] + out[x]

    def reference_point(i, _):
        lhs = lhs_keys(kfirst[i // 2])
        rows = lax.broadcasted_iota(jnp.int32, (16, BLK), 0)
        for t in range(pairs):
            top = jnp.max(dot(lhs, q_scr[i * pairs + t]), axis=0, keepdims=True)
            q_scr[i * pairs + t, pl.ds(BLK // 2, 16)] = jnp.where(rows == 0, -top, 0.0).astype(BF16)
        return 0
    lax.fori_loop(0, tiles // pairs, reference_point, 0)

    def get_ready(p):
        dev, j = ring.piece(p)

        @pl.when(p < 4)
        def _():
            start(load_piece(True, p, me, j))

        @pl.when(p >= 4)
        def _():
            recv_wait(p, dev, j)
            start(load_piece(False, p, dev, j))

        for s, at in enumerate(new_steps):
            @pl.when(p == at)
            def _():
                new_step(s + 1)
        for s, at in enumerate(new_parts):
            @pl.when(p == at)
            def _():
                for side in SIDES:
                    nwait(s + 1, side, True)
                if s == 0:
                    for c in send_new(False, sib, 0, 4, 0, 4 * hops, me):
                        c.wait_recv()

        @pl.when(new_part(p) >= 0)
        def _():
            each_load(new_part(p), lambda c: c.start())
        r, i = ring.round_of(jnp.maximum(p, 8))

        @pl.when((p >= 8) & (i < 2))
        def _():
            copies = send_piece(False, dev, j, sib_sem.at[i, lax.rem(r, 2)], p + 2, sib)

            @pl.when(r > 2)
            def _():
                for c in copies:
                    c.wait_send()
            start(copies)

        @pl.when((p >= 8) & (i == 0) & (r > 1) & (r + 2 <= rounds))
        def _():
            @pl.when(r == 2)
            def _():
                own_slot(r + 2)

            @pl.when(r > 2)
            def _():
                for side in SIDES:
                    copies = slot_copies(r + 2, side, False, *ring.far(me, r - 2, side))
                    for c in copies:
                        c.wait_send()
                    start(copies)

    def run_phase(p, _):
        dev, j = ring.piece(p)

        def ready(q, _):
            get_ready(q)
            return 0
        last = phases - 4
        lax.fori_loop(jnp.where(p == last, p, p + 1), jnp.where(p == last - 1, p + 1, jnp.minimum(p + 2, phases)), ready, 0)
        for c in load_piece(False, p, dev, j):
            c.wait()

        @pl.when(new_part(p) >= 0)
        def _():
            run_new(new_part(p))
        slot = lax.rem(p, 4)
        t0 = (j // 2) * head_tiles
        attend([(t0 + 2 * u, lambda k=k: kslot[slot, k], lambda k=k: vslot[slot, k], None, k == 0, k == nsb - 1)
                for u in range(pairs) for k in range(nsb)])
        return 0

    quad = me // 4
    quads = n // 4

    def new_part(p):
        part = const(-1)
        for s, at in enumerate(new_parts):
            part = jnp.where(p == at, s, part)
        return part

    def part_quad(part):
        near = jnp.where(lax.rem(me // 2, 2) == 0, -1, 1)
        step = jnp.where(part == 1, near, jnp.where(part == 2, -near, part // 3 * 2))
        return lax.rem(quad + step + quads, quads)

    def each_load(part, do):
        m = part_quad(part)

        def load(d, _):
            dev = 4 * m + d

            @pl.when(dev != me)
            def _():
                do(pltpu.make_async_copy(nk_all.at[dev], nkslot.at[dev], nload_sem.at[d, 0]))
                do(pltpu.make_async_copy(nv_all.at[dev], nvslot.at[dev], nload_sem.at[d, 1]))
            return 0
        lax.fori_loop(0, 4, load, 0)

    def run_new(part):
        m = part_quad(part)
        each_load(part, lambda c: c.wait())
        rowcol = (lax.broadcasted_iota(jnp.int32, (BLK, BLK), 0) - lax.broadcasted_iota(jnp.int32, (BLK, BLK), 1))

        def group(v, masked):
            low_tile = (v == 0) & masked | (part > 0) & (v == 1) & (m < quad)
            late_keys = (v == 2) | (part > 0) & (v == 1) & (m > quad)
            own = jnp.where(low_tile, me, 2 * n - 1 - me)
            block0 = 4 * jnp.where(late_keys, 2 * quads - 1 - m, m)
            blocks = []
            for h in SIDES:
                t0 = h * head_tiles + jnp.where(low_tile, 0, head_tiles // 2)
                for trio in range(pairs // 2):
                    for k in range(4):
                        block = block0 + k
                        at = jnp.where(late_keys, 2 * n - 1 - block, block)
                        i = 2 * h + late_keys.astype(jnp.int32)
                        blocks.append((t0 + 2 * trio, lambda at=at, i=i: nkslot[at, i], lambda at=at, i=i: nvslot[at, i],
                                       rowcol <= (own - block) * BLK if masked else None, k == 0, k == 3))
            attend(blocks)
            return 0

        @pl.when(part == 0)
        def _():
            lax.fori_loop(0, 2, lambda v, _: group(2 * v, True), 0)
        lax.fori_loop(jnp.where(part == 0, 1, 0), 2, lambda v, _: group(v, False), 0)

    new_steps = [8 * s + 9 for s in range(hops)] if hops == 4 else [5, 7]
    new_parts = [13, 22, 29, 37] if hops == 4 else [8, 10]
    lax.fori_loop(0, phases, run_phase, 0)

    for c in kept:
        c.wait()
    for idx, num in enumerate(nsends):
        for c in send_new(True, me, 0, num, idx, 0, me):
            c.wait_send()
    def drain(sem):
        for c in send_piece(True, me, 0, sem, 4, me):
            c.wait_send()
    for side in SIDES:
        for slot in range(4):
            drain(way_sem.at[side, slot])
        for slot in SIDES:
            drain(sib_sem.at[side, slot])
    for slot in range(4):
        drain(own_sib_sem.at[slot])


def output_kernel(n, nsb, pairs, scale, x_ref, acc_ref, l_ref, wo_ref, q_all, k_in, k_all, v_all, nk_all, nv_all,
                  y_ref, o_scr, qbuf, kbuf, vbuf, m_scr, l_scr, acc_scr, sem):
    me = lax.axis_index("cp")
    tiles = acc_ref.shape[0]
    head_tiles = tiles // 2
    head_dim = BLK // 2

    def put(t, o_t):
        h, upper, g = t // head_tiles, lax.rem(t, head_tiles) // pairs, lax.rem(t, pairs)
        rows = pl.ds(pl.multiple_of(upper * BLK, BLK), BLK)
        columns = pl.ds(pl.multiple_of((h * pairs + g) * head_dim, head_dim), head_dim)
        o_scr[rows, columns] = o_t.T.astype(BF16)

    def faults_of(t):
        denom = jnp.sum(l_ref[t], axis=0, keepdims=True)
        acc = acc_ref[t]
        fine = (jnp.abs(acc) < jnp.inf) & (denom > 2.0 ** -60) & (denom < 2.0 ** 100)
        faults = jnp.where(fine, 0.0, 1.0).reshape(head_dim // 8, 8, BLK).sum(axis=0)
        return acc * (1.0 / denom), faults

    def some(i, faults):
        for g in range(pairs):
            o_t, more = faults_of(i * pairs + g)
            put(i * pairs + g, o_t)
            faults = faults + more
        return faults
    faults = lax.fori_loop(0, tiles // pairs, some, jnp.zeros((8, BLK), F32))

    @pl.when(jnp.sum(faults) > 0.0)
    def _():
        def tile(t, _):
            @pl.when(jnp.sum(faults_of(t)[1]) > 0.0)
            def _():
                h = t // head_tiles
                upper = lax.rem(t, head_tiles) // pairs
                own = jnp.where(upper == 1, 2 * n - 1 - me, me)
                m_scr[...] = jnp.full(m_scr.shape, NEG, F32)
                l_scr[...] = jnp.zeros_like(l_scr)
                acc_scr[...] = jnp.zeros_like(acc_scr)
                queries = pltpu.make_async_copy(q_all.at[t], qbuf, sem.at[2])
                queries.start()
                queries.wait()

                def fetch(k_src, v_src):
                    copies = (pltpu.make_async_copy(k_src, kbuf, sem.at[0]), pltpu.make_async_copy(v_src, vbuf, sem.at[1]))
                    for c in copies:
                        c.start()
                    for c in copies:
                        c.wait()

                def step(limit):
                    s = dot(kbuf[...], qbuf[...]) * scale
                    rows = lax.broadcasted_iota(jnp.int32, s.shape, 0) - lax.broadcasted_iota(jnp.int32, s.shape, 1)
                    s = jnp.where(rows <= limit, s, -jnp.inf)
                    m_old = m_scr[...]
                    m_new = jnp.maximum(m_old, jnp.max(s, axis=0, keepdims=True))
                    e = jnp.exp(s - m_new)
                    old = jnp.exp(m_old - m_new)
                    m_scr[...] = m_new
                    l_scr[...] = l_scr[...] * old + jnp.sum(e, axis=0, keepdims=True)
                    acc_scr[...] = acc_scr[...] * old + dot(vbuf[...], e.astype(BF16))

                def cached(b, _):
                    dev, rem = b // (2 * nsb), lax.rem(b, 2 * nsb)
                    j, k = 2 * h + rem // nsb, lax.rem(rem, nsb)

                    @pl.when(dev == me)
                    def _():
                        fetch(k_in.at[j, k], v_all.at[dev, j, k])

                    @pl.when(dev != me)
                    def _():
                        fetch(k_all.at[dev, j, k], v_all.at[dev, j, k])
                    step(0 * me + BLK)
                    return 0

                def new(b, _):
                    dev = jnp.where(b < n, b, 2 * n - 1 - b)
                    j = 2 * h + (b >= n).astype(jnp.int32)
                    fetch(nk_all.at[dev, j], nv_all.at[dev, j])
                    step((own - b) * BLK)
                    return 0
                lax.fori_loop(0, 2 * nsb * n, cached, 0)
                lax.fori_loop(0, own + 1, new, 0)
                put(t, acc_scr[...] / l_scr[...])
            return 0
        lax.fori_loop(0, tiles, tile, 0)
    width = min(512, wo_ref.shape[1])

    def project(c, _):
        columns = pl.ds(pl.multiple_of(c * width, width), width)
        y_ref[:, columns] = (x_ref[:, columns].astype(F32) + dot(o_scr[...], wo_ref[:, columns])).astype(BF16)
        return 0
    lax.fori_loop(0, wo_ref.shape[1] // width, project, 0)


def in_hbm(a):
    return pltpu.with_memory_space_constraint(a, HBM)


def solution(mesh):
    n = mesh.shape["cp"]

    def local_step(x_loc, pos_loc, k_loc, v_loc, w_q, w_k, w_v, w_o):
        tok_dev, model_dim = x_loc.shape
        cache_dev, kv_heads, head_dim = k_loc.shape
        q_heads = w_q.shape[1] // head_dim
        group = q_heads // kv_heads
        half = head_dim // 2
        nsb = cache_dev // (2 * BLK)
        pairs = group
        tiles = 2 * q_heads
        inv_freq = jnp.power(jnp.float32(ROPE_BASE), -(jnp.arange(half, dtype=F32) * 2.0 / head_dim))
        angles = pos_loc.astype(F32)[:, None] * inv_freq[None, :]
        cos_a, sin_a = jnp.cos(angles), jnp.sin(angles)
        cos_t = jnp.concatenate([cos_a, cos_a], axis=1)
        sin_t = jnp.concatenate([-sin_a, sin_a], axis=1)

        k_pieces = jnp.transpose(k_loc, (1, 0, 2)).reshape(4, nsb, BLK, head_dim)
        v_pieces = jnp.transpose(v_loc, (1, 0, 2)).reshape(4, nsb, BLK, head_dim)

        hops = n // 4
        rounds = 4 * (hops - 1) + 2
        phases = 8 + 4 * rounds
        vmem_spec = pl.BlockSpec(memory_space=VMEM)
        dma = pltpu.SemaphoreType.DMA
        scale2 = math.log2(math.e) / math.sqrt(head_dim)
        n_new_sends = 3 + 2 * (hops - 1) + 2 * hops
        hbm_spec = pl.BlockSpec(memory_space=HBM)
        acc, l, q_all, k_all, v_all, nk_all, nv_all = pl.pallas_call(
            functools.partial(attend_kernel, n, nsb, pairs, scale2),
            out_shape=(
                jax.ShapeDtypeStruct((tiles, head_dim, BLK), F32),
                jax.ShapeDtypeStruct((tiles, 8, BLK), F32),
                HBM((tiles, head_dim, BLK), BF16),
                HBM((n,) + k_pieces.shape, BF16),
                HBM((n, 4, nsb, head_dim, BLK), BF16),
                HBM((n, 4, BLK, head_dim), BF16),
                HBM((n, 4, head_dim, BLK), BF16),
            ),
            in_specs=[vmem_spec, hbm_spec] + [vmem_spec] * 4 + [hbm_spec, vmem_spec],
            out_specs=(vmem_spec, vmem_spec) + (hbm_spec,) * 5,
            scratch_shapes=[
                VMEM((tiles, BLK, BLK), BF16),
                VMEM((4, nsb, BLK, head_dim), BF16),
                VMEM((4, nsb, head_dim, BLK), BF16),
                VMEM((n, 4, BLK, head_dim), BF16),
                VMEM((n, 4, head_dim, BLK), BF16),
                VMEM((2, 4, BLK, BLK), BF16),
                VMEM((2, BLK, head_dim), BF16),
                VMEM((16, head_dim), BF16),
                VMEM(w_q.shape, BF16),
                VMEM((4, nsb, head_dim, BLK), BF16),
                dma((phases - 4, 2)),
                dma((2, 4, 2)),
                dma((2, 2, 2)),
                dma((4, 2)),
                dma((4 * hops + 1, 2)),
                dma((n_new_sends, 2)),
                dma((4, 2)),
                dma((7,)),
                dma((4, 2)),
            ],
            compiler_params=pltpu.CompilerParams(collective_id=0, has_side_effects=True, vmem_limit_bytes=36 * 2 ** 20),
            name="ring_attention",
        )(x_loc, in_hbm(w_q), w_k, w_v, cos_t, sin_t, in_hbm(k_pieces), v_pieces)

        return pl.pallas_call(
            functools.partial(output_kernel, n, nsb, pairs, 1.0 / math.sqrt(head_dim)),
            out_shape=jax.ShapeDtypeStruct((tok_dev, model_dim), BF16),
            in_specs=[vmem_spec] * 4 + [hbm_spec] * 6,
            out_specs=vmem_spec,
            scratch_shapes=[VMEM((tok_dev, q_heads * head_dim), BF16), VMEM((head_dim, BLK), BF16),
                            VMEM((BLK, head_dim), BF16), VMEM((head_dim, BLK), BF16), VMEM((1, BLK), F32), VMEM((1, BLK), F32),
                            VMEM((head_dim, BLK), F32), dma((3,))],
            compiler_params=pltpu.CompilerParams(vmem_limit_bytes=16 * 2 ** 20),
            name="output",
        )(x_loc, acc, l, w_o, *(in_hbm(a) for a in (q_all, k_pieces, k_all, v_all, nk_all, nv_all)))

    tok_spec = P(("data", "cp"), None)
    pos_spec = P(("data", "cp"))
    cache_spec = P(("data", "cp"), None, None)
    return jax.shard_map(local_step, mesh=mesh, in_specs=(tok_spec, pos_spec, cache_spec, cache_spec, P(), P(), P(), P()), out_specs=tok_spec, check_vma=False)
```

```python
import functools
import math
import jax
import jax.numpy as jnp
from jax import lax
from jax.experimental import pallas as pl
from jax.experimental.pallas import tpu as pltpu
from jax.sharding import PartitionSpec as P

ROPE_BASE = 500000.0
BLK = 256
HBM = pltpu.HBM
VMEM = pltpu.VMEM
BF16 = jnp.bfloat16
F32 = jnp.float32
MESH_ID = pl.DeviceIdType.MESH
NEG = -1e30
SIDES = (0, 1)
LAG = 2


class Ring:
    def __init__(self, n):
        self.n = n
        me = lax.axis_index("cp")
        self.me = me
        self.sib = me + 1 - 2 * lax.rem(me, 2)
        self.right = lax.rem(me + 2, n)
        self.left = lax.rem(me + n - 2, n)
        self.hops = n // 4
        self.rounds = 4 * (self.hops - 1) + 2
        self.phases = 8 + 4 * self.rounds
        self.direct = self.rounds - 3

    def round_of(self, p):
        return (p - 8) // 4 + 1, lax.rem(p - 8, 4)

    def slot(self, p):
        r, i = self.round_of(jnp.maximum(p, 8))
        return jnp.where(self.arrives_direct(p), 4 + 2 * (r - self.direct) + i, lax.rem(p, 4))

    def arrives_direct(self, p):
        r, i = self.round_of(jnp.maximum(p, 8))
        return (i < 2) & (r >= self.direct) & (p >= 8)

    def far(self, base, r, side):
        s = (r - 1) // 4 + 1
        return lax.rem(base + self.n + (2 * side - 1) * 2 * s, self.n), lax.rem(r - 1 + 2 * side, 4)

    def piece(self, p):
        r, i = self.round_of(jnp.maximum(p, 8))
        dev, j = self.far(jnp.where(i >= 2, self.sib, self.me), r, lax.rem(i, 2))
        early_dev = jnp.where(p >= 4, self.sib, self.me)
        return jnp.where(p < 8, early_dev, dev), jnp.where(p < 8, lax.rem(p, 4), j)


def dot(a, b):
    return jnp.dot(a, b, preferred_element_type=F32)


def attend_kernel(n, nsb, pairs, scale2, x_in, wq_in, wk_in, wv_in, cos_ref, sin_ref, k_in, vn_ref,
                  acc_out, l_out, q_all, k_all, v_all, nk_all, nv_all,
                  q_scr, kslot, vslot, nkslot, nvslot, p_scr, kfirst, ones_scr, x_ref, wk_ref, wv_ref, wq_scr, vt_scr,
                  recv_sem, way_sem, sib_sem, own_sib_sem, nrecv_sem, nsend_sem, load_sem, keep_sem, misc_sem, nload_sem):
    ring = Ring(n)
    me, sib, right, left, hops = ring.me, ring.sib, ring.right, ring.left, ring.hops
    rounds, phases, direct = ring.rounds, ring.phases, ring.direct
    tiles = q_scr.shape[0]
    head_tiles = tiles // 2

    def const(value):
        return 0 * me + value

    def send(src, dst, send_sem, recv, to):
        return pltpu.make_async_remote_copy(src_ref=src, dst_ref=dst, send_sem=send_sem, recv_sem=recv,
                                            device_id={"cp": to}, device_id_type=MESH_ID)

    def send_piece(from_own, dev, j, pair_sem, phase, to, src_slot=None, dst_slot=None):
        kdst, vdst = k_all.at[dev, j], v_all.at[dev, j]
        ksrc, vsrc = (k_in.at[j] if from_own else kdst), vdst
        if src_slot is not None:
            ksrc, vsrc = kslot.at[src_slot], vslot.at[src_slot]
        if dst_slot is not None:
            kdst, vdst = kslot.at[dst_slot], vslot.at[dst_slot]
        return (send(ksrc, kdst, pair_sem.at[0], recv_sem.at[phase - 4, 0], to),
                send(vsrc, vdst, pair_sem.at[1], recv_sem.at[phase - 4, 1], to))

    def send_new(from_own, dev, lo, num, idx, ridx, to):
        ksrc = (nkslot if from_own else nk_all).at[dev, pl.ds(lo, num)]
        vsrc = (nvslot if from_own else nv_all).at[dev, pl.ds(lo, num)]
        return (send(ksrc, nk_all.at[dev, pl.ds(lo, num)], nsend_sem.at[idx, 0], nrecv_sem.at[ridx, 0], to),
                send(vsrc, nv_all.at[dev, pl.ds(lo, num)], nsend_sem.at[idx, 1], nrecv_sem.at[ridx, 1], to))

    def start(copies):
        for c in copies:
            c.start()

    def recv_wait(phase, dev, j):
        for c in send_piece(False, dev, j, own_sib_sem.at[0], phase, me):
            c.wait_recv()

    def nleft(s):
        return lax.rem(me + n - 2 * s, n)

    def nright(s):
        return lax.rem(me + 2 * s, n)

    def nwait(s, side, from_sib):
        base = sib if from_sib else me
        dev = lax.rem(base + (2 * s if side else n - 2 * s), n)
        lo, num = (0, 4) if s < hops else (2 * side, 2)
        for c in send_new(False, dev, lo, num, 0, 2 * (s - 1) + side + (2 * hops if from_sib else 0), me):
            c.wait_recv()

    nsends = []

    def new_step(s):
        for side in SIDES:
            nwait(s, side, False)
        for side in SIDES:
            dev = nright(s) if side else nleft(s)
            if s < hops:
                lo, num = (0, 4) if s + 1 < hops else (2 * side, 2)
                idx = len(nsends)
                copies = send_new(False, dev, lo, num, idx, 2 * s + side, left if side else right)
                start(copies)
                nsends.append(num)
            lo, num = (0, 4) if s < hops else (2 * side, 2)
            idx = len(nsends)
            copies = send_new(False, dev, lo, num, idx, 2 * hops + 2 * (s - 1) + side, sib)
            start(copies)
            nsends.append(num)

    then = [pltpu.make_async_copy(wq_in, wq_scr, misc_sem.at[0])]
    then += [pltpu.make_async_copy(k_in.at[2 * h, 0], kfirst.at[h], misc_sem.at[1 + h]) for h in SIDES]
    first = [pltpu.make_async_copy(a, b, misc_sem.at[7 + i])
             for i, (a, b) in enumerate(((x_in, x_ref), (wk_in, wk_ref), (wv_in, wv_ref)))]
    start(first)
    start(then)

    barrier = pltpu.get_barrier_semaphore()
    for other in (left, right, sib):
        pl.semaphore_signal(barrier, inc=1, device_id={"cp": other}, device_id_type=MESH_ID)
    pl.semaphore_wait(barrier, 3)

    def own_slot(slot):
        for side in SIDES:
            start(slot_copies(const(slot), side, True, me, (slot - 1 + 2 * side) % 4, slot >= direct))

    def slot_copies(slot, side, own, dev, j, to_vmem=False):
        phase = 4 + 4 * slot + side
        return send_piece(own, dev, j, way_sem.at[side, lax.rem(slot, 4)], phase, (right, left)[side],
                          dst_slot=ring.slot(phase) if to_vmem else None)

    first_round = [slot_copies(const(1), side, True, me, 2 * side) for side in SIDES]
    first_round += [send_piece(True, me, j, own_sib_sem.at[j], 4 + j, sib) for j in range(4)]
    start([c[0] for c in first_round])

    def load_piece(own, p, dev, j):
        ksrc = k_in.at[j] if own else k_all.at[dev, j]
        vsrc = v_all.at[dev, j]
        slot = lax.rem(p, 4)
        return (pltpu.make_async_copy(ksrc, kslot.at[slot], load_sem.at[slot, 0]),
                pltpu.make_async_copy(vsrc, vslot.at[slot], load_sem.at[slot, 1]))

    def keep_piece(slot, dev, j):
        return (pltpu.make_async_copy(kslot.at[slot], k_all.at[dev, j], keep_sem.at[slot - 4, 0]),
                pltpu.make_async_copy(vslot.at[slot], v_all.at[dev, j], keep_sem.at[slot - 4, 1]))

    ones_scr[...] = jnp.where(lax.broadcasted_iota(jnp.int32, ones_scr.shape, 1) == 0, 1.0, 0.0).astype(BF16)

    def clear(t, _):
        q_scr[t, pl.ds(BLK // 2, BLK // 2)] = jnp.zeros((BLK // 2, BLK), BF16)
        acc_out[t] = jnp.zeros(acc_out.shape[1:], F32)
        l_out[t] = jnp.zeros(l_out.shape[1:], F32)
        return 0
    lax.fori_loop(0, tiles, clear, 0)

    def transpose(j, _):
        for k in range(nsb):
            vt_scr[j, k] = vn_ref[j, k].T
        return 0
    lax.fori_loop(0, 4, transpose, 0)
    own_values = pltpu.make_async_copy(vt_scr, v_all.at[me], misc_sem.at[3])
    own_values.start()
    for c in first:
        c.wait()

    head_dim = BLK // 2

    def turned(u):
        u = u.astype(BF16).astype(F32)
        return (u * cos_ref[...] + pltpu.roll(u, head_dim // 2, 1) * sin_ref[...]).astype(BF16)

    new_k, new_v = dot(x_ref[...], wk_ref[...]), dot(x_ref[...], wv_ref[...])
    for h in SIDES:
        keys = turned(new_k[:, h * head_dim:(h + 1) * head_dim])
        values = new_v[:, h * head_dim:(h + 1) * head_dim].T.astype(BF16)
        for half in SIDES:
            nkslot[me, 2 * h + half] = keys[half * BLK:(half + 1) * BLK]
            nvslot[me, 2 * h + half] = values[:, half * BLK:(half + 1) * BLK]
    own_values.wait()
    start([c[1] for c in first_round])
    start(load_piece(True, const(0), me, 0))
    for c in then:
        c.wait()
    heads = 4

    def project(c, _):
        width = heads * head_dim
        z = dot(x_ref[...], wq_scr[:, pl.ds(pl.multiple_of(c * width, width), width)])
        for i in range(heads):
            head = c * heads + i
            t = (head // pairs) * head_tiles + lax.rem(head, pairs)
            u = turned(z[:, i * head_dim:(i + 1) * head_dim]).astype(F32).T.astype(BF16)
            for half in SIDES:
                q_scr[t + half * pairs, pl.ds(0, head_dim)] = u[:, half * BLK:(half + 1) * BLK]
        return 0
    lax.fori_loop(0, tiles // (2 * heads), project, 0)

    for other, ridx in ((right, 0), (left, 1), (sib, 4 * hops)):
        start(send_new(True, me, 0, 4, len(nsends), ridx, other))
        nsends.append(4)
    own_slot(2)
    own_slot(3)
    kept = [pltpu.make_async_copy(q_scr.at[:, pl.ds(0, head_dim)], q_all, misc_sem.at[4]),
            pltpu.make_async_copy(nkslot.at[me], nk_all.at[me], misc_sem.at[5]),
            pltpu.make_async_copy(nvslot.at[me], nv_all.at[me], misc_sem.at[6])]
    start(kept)

    def lhs_keys(keys):
        ones = ones_scr[...]
        return jnp.concatenate([keys, jnp.concatenate([ones] * (BLK // 16), axis=0)], axis=1)

    def attend(blocks):
        def scores(b):
            lhs = lhs_keys(b[1]())
            return [dot(lhs, q_scr[b[0] + x]) for x in SIDES]

        ahead = scores(blocks[0])
        sums, out = [None, None], [None, None]
        for i in range(len(blocks) + LAG):
            now = ahead
            if i + 1 < len(blocks):
                ahead = scores(blocks[i + 1])
            if i < len(blocks):
                t, _, _, bias, first, last = blocks[i]
                for x in SIDES:
                    s = now[x] * scale2
                    e = jnp.exp2(s if bias is None else jnp.where(bias, s, NEG))
                    p_scr[x, i % 4] = e.astype(BF16)
                    part = e.reshape(BLK // 8, 8, BLK).sum(axis=0)
                    sums[x] = part if first else sums[x] + part
                    if last:
                        l_out[t + x] = l_out[t + x] + sums[x]
            if i >= LAG:
                t, _, values, _, first, last = blocks[i - LAG]
                v = values()
                for x in SIDES:
                    part = dot(v, p_scr[x, (i - LAG) % 4])
                    out[x] = part if first else out[x] + part
                    if last:
                        acc_out[t + x] = acc_out[t + x] + out[x]

    def reference_point(i, _):
        lhs = lhs_keys(kfirst[i // 2])
        rows = lax.broadcasted_iota(jnp.int32, (16, BLK), 0)
        for t in range(pairs):
            top = jnp.max(dot(lhs, q_scr[i * pairs + t]), axis=0, keepdims=True)
            q_scr[i * pairs + t, pl.ds(BLK // 2, 16)] = jnp.where(rows == 0, -top, 0.0).astype(BF16)
        return 0
    lax.fori_loop(0, tiles // pairs, reference_point, 0)

    def get_ready(p):
        dev, j = ring.piece(p)
        arrived = ring.arrives_direct(p)

        @pl.when(p < 4)
        def _():
            start(load_piece(True, p, me, j))

        @pl.when(p >= 4)
        def _():
            recv_wait(p, dev, j)

        @pl.when((p >= 4) & ~arrived)
        def _():
            start(load_piece(False, p, dev, j))

        @pl.when(arrived)
        def _():
            start(keep_piece(ring.slot(p), dev, j))

        for s, at in enumerate(new_steps):
            @pl.when(p == at)
            def _():
                new_step(s + 1)
        for s, at in enumerate(new_parts):
            @pl.when(p == at)
            def _():
                for side in SIDES:
                    nwait(s + 1, side, True)
                if s == 0:
                    for c in send_new(False, sib, 0, 4, 0, 4 * hops, me):
                        c.wait_recv()

        @pl.when(new_part(p) >= 0)
        def _():
            each_load(new_part(p), lambda c: c.start())
        r, i = ring.round_of(jnp.maximum(p, 8))

        @pl.when((p >= 8) & (i < 2))
        def _():
            sem = sib_sem.at[i, lax.rem(r, 2)]

            @pl.when(r > 2)
            def _():
                for c in send_piece(False, dev, j, sem, p + 2, sib):
                    c.wait_send()

            @pl.when(~arrived)
            def _():
                start(send_piece(False, dev, j, sem, p + 2, sib))

            @pl.when(arrived)
            def _():
                start(send_piece(False, dev, j, sem, p + 2, sib, src_slot=ring.slot(p)))

        @pl.when((p >= 8) & (i == 0) & (r > 1) & (r + 2 <= rounds))
        def _():
            @pl.when(r == 2)
            def _():
                own_slot(4)

            for to_vmem in (False, True):
                @pl.when((r > 2) & ((r + 2 >= direct) == to_vmem))
                def _():
                    for side in SIDES:
                        copies = slot_copies(r + 2, side, False, *ring.far(me, r - 2, side), to_vmem)
                        for c in copies:
                            c.wait_send()
                        start(copies)

    def run_phase(p, _):
        dev, j = ring.piece(p)

        def ready(q, _):
            get_ready(q)
            return 0
        late, late_next = ((lax.rem(q, 4) == 0) & ring.arrives_direct(q) for q in (p, p + 1))
        lax.fori_loop(jnp.where(late, p, p + 1), jnp.where(late_next, p + 1, jnp.minimum(p + 2, phases)), ready, 0)

        @pl.when(~ring.arrives_direct(p))
        def _():
            for c in load_piece(False, p, dev, j):
                c.wait()

        @pl.when(new_part(p) >= 0)
        def _():
            run_new(new_part(p))
        slot = ring.slot(p)
        t0 = (j // 2) * head_tiles
        attend([(t0 + 2 * u, lambda k=k: kslot[slot, k], lambda k=k: vslot[slot, k], None, k == 0, k == nsb - 1)
                for u in range(pairs) for k in range(nsb)])
        return 0

    quad = me // 4
    quads = n // 4

    def new_part(p):
        part = const(-1)
        for s, at in enumerate(new_parts):
            part = jnp.where(p == at, s, part)
        return part

    def part_quad(part):
        near = jnp.where(lax.rem(me // 2, 2) == 0, -1, 1)
        step = jnp.where(part == 1, near, jnp.where(part == 2, -near, part // 3 * 2))
        return lax.rem(quad + step + quads, quads)

    def each_load(part, do):
        m = part_quad(part)

        def load(d, _):
            dev = 4 * m + d

            @pl.when(dev != me)
            def _():
                do(pltpu.make_async_copy(nk_all.at[dev], nkslot.at[dev], nload_sem.at[d, 0]))
                do(pltpu.make_async_copy(nv_all.at[dev], nvslot.at[dev], nload_sem.at[d, 1]))
            return 0
        lax.fori_loop(0, 4, load, 0)

    def run_new(part):
        m = part_quad(part)
        each_load(part, lambda c: c.wait())
        rowcol = (lax.broadcasted_iota(jnp.int32, (BLK, BLK), 0) - lax.broadcasted_iota(jnp.int32, (BLK, BLK), 1))

        def group(v, masked):
            low_tile = (v == 0) & masked | (part > 0) & (v == 1) & (m < quad)
            late_keys = (v == 2) | (part > 0) & (v == 1) & (m > quad)
            own = jnp.where(low_tile, me, 2 * n - 1 - me)
            block0 = 4 * jnp.where(late_keys, 2 * quads - 1 - m, m)
            blocks = []
            for h in SIDES:
                t0 = h * head_tiles + jnp.where(low_tile, 0, head_tiles // 2)
                for trio in range(pairs // 2):
                    for k in range(4):
                        block = block0 + k
                        at = jnp.where(late_keys, 2 * n - 1 - block, block)
                        i = 2 * h + late_keys.astype(jnp.int32)
                        blocks.append((t0 + 2 * trio, lambda at=at, i=i: nkslot[at, i], lambda at=at, i=i: nvslot[at, i],
                                       rowcol <= (own - block) * BLK if masked else None, k == 0, k == 3))
            attend(blocks)
            return 0

        @pl.when(part == 0)
        def _():
            lax.fori_loop(0, 2, lambda v, _: group(2 * v, True), 0)
        lax.fori_loop(jnp.where(part == 0, 1, 0), 2, lambda v, _: group(v, False), 0)

    new_steps = [8 * s + 9 for s in range(hops)] if hops == 4 else [5, 7]
    new_parts = [13, 22, 29, 37] if hops == 4 else [8, 10]
    lax.fori_loop(0, phases, run_phase, 0)

    for c in kept:
        c.wait()
    for slot in range(4, kslot.shape[0]):
        for c in keep_piece(slot, me, 0):
            c.wait()
    for idx, num in enumerate(nsends):
        for c in send_new(True, me, 0, num, idx, 0, me):
            c.wait_send()
    def drain(sem):
        for c in send_piece(True, me, 0, sem, 4, me):
            c.wait_send()
    for side in SIDES:
        for slot in range(4):
            drain(way_sem.at[side, slot])
        for slot in SIDES:
            drain(sib_sem.at[side, slot])
    for slot in range(4):
        drain(own_sib_sem.at[slot])


def output_kernel(n, nsb, pairs, scale, x_ref, acc_ref, l_ref, wo_ref, q_all, k_in, k_all, v_all, nk_all, nv_all,
                  y_ref, o_scr, qbuf, kbuf, vbuf, m_scr, l_scr, acc_scr, sem):
    me = lax.axis_index("cp")
    tiles = acc_ref.shape[0]
    head_tiles = tiles // 2
    head_dim = BLK // 2

    def put(t, o_t):
        h, upper, g = t // head_tiles, lax.rem(t, head_tiles) // pairs, lax.rem(t, pairs)
        rows = pl.ds(pl.multiple_of(upper * BLK, BLK), BLK)
        columns = pl.ds(pl.multiple_of((h * pairs + g) * head_dim, head_dim), head_dim)
        o_scr[rows, columns] = o_t.T.astype(BF16)

    def faults_of(t):
        denom = jnp.sum(l_ref[t], axis=0, keepdims=True)
        acc = acc_ref[t]
        fine = (jnp.abs(acc) < jnp.inf) & (denom > 2.0 ** -60) & (denom < 2.0 ** 100)
        faults = jnp.where(fine, 0.0, 1.0).reshape(head_dim // 8, 8, BLK).sum(axis=0)
        return acc * (1.0 / denom), faults

    def some(i, faults):
        for g in range(pairs):
            o_t, more = faults_of(i * pairs + g)
            put(i * pairs + g, o_t)
            faults = faults + more
        return faults
    faults = lax.fori_loop(0, tiles // pairs, some, jnp.zeros((8, BLK), F32))

    @pl.when(jnp.sum(faults) > 0.0)
    def _():
        def tile(t, _):
            @pl.when(jnp.sum(faults_of(t)[1]) > 0.0)
            def _():
                h = t // head_tiles
                upper = lax.rem(t, head_tiles) // pairs
                own = jnp.where(upper == 1, 2 * n - 1 - me, me)
                m_scr[...] = jnp.full(m_scr.shape, NEG, F32)
                l_scr[...] = jnp.zeros_like(l_scr)
                acc_scr[...] = jnp.zeros_like(acc_scr)
                queries = pltpu.make_async_copy(q_all.at[t], qbuf, sem.at[2])
                queries.start()
                queries.wait()

                def fetch(k_src, v_src):
                    copies = (pltpu.make_async_copy(k_src, kbuf, sem.at[0]), pltpu.make_async_copy(v_src, vbuf, sem.at[1]))
                    for c in copies:
                        c.start()
                    for c in copies:
                        c.wait()

                def step(limit):
                    s = dot(kbuf[...], qbuf[...]) * scale
                    rows = lax.broadcasted_iota(jnp.int32, s.shape, 0) - lax.broadcasted_iota(jnp.int32, s.shape, 1)
                    s = jnp.where(rows <= limit, s, -jnp.inf)
                    m_old = m_scr[...]
                    m_new = jnp.maximum(m_old, jnp.max(s, axis=0, keepdims=True))
                    e = jnp.exp(s - m_new)
                    old = jnp.exp(m_old - m_new)
                    m_scr[...] = m_new
                    l_scr[...] = l_scr[...] * old + jnp.sum(e, axis=0, keepdims=True)
                    acc_scr[...] = acc_scr[...] * old + dot(vbuf[...], e.astype(BF16))

                def cached(b, _):
                    dev, rem = b // (2 * nsb), lax.rem(b, 2 * nsb)
                    j, k = 2 * h + rem // nsb, lax.rem(rem, nsb)

                    @pl.when(dev == me)
                    def _():
                        fetch(k_in.at[j, k], v_all.at[dev, j, k])

                    @pl.when(dev != me)
                    def _():
                        fetch(k_all.at[dev, j, k], v_all.at[dev, j, k])
                    step(0 * me + BLK)
                    return 0

                def new(b, _):
                    dev = jnp.where(b < n, b, 2 * n - 1 - b)
                    j = 2 * h + (b >= n).astype(jnp.int32)
                    fetch(nk_all.at[dev, j], nv_all.at[dev, j])
                    step((own - b) * BLK)
                    return 0
                lax.fori_loop(0, 2 * nsb * n, cached, 0)
                lax.fori_loop(0, own + 1, new, 0)
                put(t, acc_scr[...] / l_scr[...])
            return 0
        lax.fori_loop(0, tiles, tile, 0)
    width = min(512, wo_ref.shape[1])

    def project(c, _):
        columns = pl.ds(pl.multiple_of(c * width, width), width)
        y_ref[:, columns] = (x_ref[:, columns].astype(F32) + dot(o_scr[...], wo_ref[:, columns])).astype(BF16)
        return 0
    lax.fori_loop(0, wo_ref.shape[1] // width, project, 0)


def in_hbm(a):
    return pltpu.with_memory_space_constraint(a, HBM)


def solution(mesh):
    n = mesh.shape["cp"]

    def local_step(x_loc, pos_loc, k_loc, v_loc, w_q, w_k, w_v, w_o):
        tok_dev, model_dim = x_loc.shape
        cache_dev, kv_heads, head_dim = k_loc.shape
        q_heads = w_q.shape[1] // head_dim
        group = q_heads // kv_heads
        half = head_dim // 2
        nsb = cache_dev // (2 * BLK)
        pairs = group
        tiles = 2 * q_heads
        inv_freq = jnp.power(jnp.float32(ROPE_BASE), -(jnp.arange(half, dtype=F32) * 2.0 / head_dim))
        angles = pos_loc.astype(F32)[:, None] * inv_freq[None, :]
        cos_a, sin_a = jnp.cos(angles), jnp.sin(angles)
        cos_t = jnp.concatenate([cos_a, cos_a], axis=1)
        sin_t = jnp.concatenate([-sin_a, sin_a], axis=1)

        k_pieces = jnp.transpose(k_loc, (1, 0, 2)).reshape(4, nsb, BLK, head_dim)
        v_pieces = jnp.transpose(v_loc, (1, 0, 2)).reshape(4, nsb, BLK, head_dim)

        hops = n // 4
        rounds = 4 * (hops - 1) + 2
        phases = 8 + 4 * rounds
        vmem_spec = pl.BlockSpec(memory_space=VMEM)
        dma = pltpu.SemaphoreType.DMA
        scale2 = math.log2(math.e) / math.sqrt(head_dim)
        n_new_sends = 3 + 2 * (hops - 1) + 2 * hops
        hbm_spec = pl.BlockSpec(memory_space=HBM)
        acc, l, q_all, k_all, v_all, nk_all, nv_all = pl.pallas_call(
            functools.partial(attend_kernel, n, nsb, pairs, scale2),
            out_shape=(
                jax.ShapeDtypeStruct((tiles, head_dim, BLK), F32),
                jax.ShapeDtypeStruct((tiles, 8, BLK), F32),
                HBM((tiles, head_dim, BLK), BF16),
                HBM((n,) + k_pieces.shape, BF16),
                HBM((n, 4, nsb, head_dim, BLK), BF16),
                HBM((n, 4, BLK, head_dim), BF16),
                HBM((n, 4, head_dim, BLK), BF16),
            ),
            in_specs=[hbm_spec] * 4 + [vmem_spec] * 2 + [hbm_spec, vmem_spec],
            out_specs=(vmem_spec, vmem_spec) + (hbm_spec,) * 5,
            scratch_shapes=[
                VMEM((tiles, BLK, BLK), BF16),
                VMEM((12, nsb, BLK, head_dim), BF16),
                VMEM((12, nsb, head_dim, BLK), BF16),
                VMEM((n, 4, BLK, head_dim), BF16),
                VMEM((n, 4, head_dim, BLK), BF16),
                VMEM((2, 4, BLK, BLK), BF16),
                VMEM((2, BLK, head_dim), BF16),
                VMEM((16, head_dim), BF16),
                VMEM(x_loc.shape, BF16),
                VMEM(w_k.shape, BF16),
                VMEM(w_v.shape, BF16),
                VMEM(w_q.shape, BF16),
                VMEM((4, nsb, head_dim, BLK), BF16),
                dma((phases - 4, 2)),
                dma((2, 4, 2)),
                dma((2, 2, 2)),
                dma((4, 2)),
                dma((4 * hops + 1, 2)),
                dma((n_new_sends, 2)),
                dma((4, 2)),
                dma((8, 2)),
                dma((10,)),
                dma((4, 2)),
            ],
            compiler_params=pltpu.CompilerParams(collective_id=0, has_side_effects=True, vmem_limit_bytes=44 * 2 ** 20),
            name="ring_attention",
        )(in_hbm(x_loc), in_hbm(w_q), in_hbm(w_k), in_hbm(w_v), cos_t, sin_t, in_hbm(k_pieces), v_pieces)

        return pl.pallas_call(
            functools.partial(output_kernel, n, nsb, pairs, 1.0 / math.sqrt(head_dim)),
            out_shape=jax.ShapeDtypeStruct((tok_dev, model_dim), BF16),
            in_specs=[vmem_spec] * 4 + [hbm_spec] * 6,
            out_specs=vmem_spec,
            scratch_shapes=[VMEM((tok_dev, q_heads * head_dim), BF16), VMEM((head_dim, BLK), BF16),
                            VMEM((BLK, head_dim), BF16), VMEM((head_dim, BLK), BF16), VMEM((1, BLK), F32), VMEM((1, BLK), F32),
                            VMEM((head_dim, BLK), F32), dma((3,))],
            compiler_params=pltpu.CompilerParams(vmem_limit_bytes=16 * 2 ** 20),
            name="output",
        )(x_loc, acc, l, w_o, *(in_hbm(a) for a in (q_all, k_pieces, k_all, v_all, nk_all, nv_all)))

    tok_spec = P(("data", "cp"), None)
    pos_spec = P(("data", "cp"))
    cache_spec = P(("data", "cp"), None, None)
    return jax.shard_map(local_step, mesh=mesh, in_specs=(tok_spec, pos_spec, cache_spec, cache_spec, P(), P(), P(), P()), out_specs=tok_spec, check_vma=False)
```
